32 devices in a mesh: epoch: 4 (over y, x), blend: 8 (over z, core).
Axes of the slice: x: 2, y: 2, z: 4, core: 2. Of those that a mesh axis runs over, the one named last changes fastest.
Arguments:
- visit_flux: bfloat16 [16, 32, 6, 16384], P('epoch', None, None, 'blend'), may hold values from -6 to 6
- visit_precision: bfloat16 [16, 32, 6, 16384], P('epoch', None, None, 'blend'), may hold values from 0.25 to 4
- visit_live: int32 [16, 32], P('epoch'), may hold values 0 or 1
- footprint: int32 [32, 8, 16384], P('blend', None, 'epoch'), may hold values 0 or 1
- source_count: int32 [32], P('blend'), may hold values from 1 to 8
- spectra_init: float32 [32, 8, 6], P('blend'), may hold values from 0.2 to 1.2
- morphology_init: float32 [32, 8, 16384], P('blend', None, 'epoch'), may hold values from 0 to 0.25
Outputs:
- coadd_flux: float32 [32, 6, 16384], P('blend', None, 'epoch')
- spectra: float32 [32, 8, 6], P('blend')
- morphology: float32 [32, 8, 16384], P('blend', None, 'epoch')
The draws below stay inside these ranges and needn't reach their ends.
All inputs are finite; a program needn't handle non-finite values. No bound on the sum of `visit_live` or of `footprint` on one device may be relied on, other than what follows from the above.
Results may differ from the reference program's by a relative error of at most 0.0003.
Values sent between devices are 32-bit elements; how exact they have to be, the bound alone decides.
A program may use at most 64 MiB of HBM per device.

```python
import math
import jax
import jax.numpy as jnp
from jax import lax

PIX = 16384
BANDS = 6
SRC = 8
ITERS = 2
EPOCHS = 16
BLENDS = 32


def with_ends(array, key, smallest, largest):
    dims = array.shape
    place = [jax.random.randint(jax.random.fold_in(key, axis), (), 0, dims[axis]) for axis in range(len(dims))]
    array = array.at[tuple(place)].set(smallest)
    longest = dims.index(max(dims))
    place[longest] = (place[longest] + 1) % dims[longest]
    return array.at[tuple(place)].set(largest)


def shard_levels(rng, shape, pieces, low, top_value):
    def one(position, blocks):
        draws = jax.random.uniform(jax.random.fold_in(jax.random.fold_in(rng, 6), position), (blocks,), jnp.float32, low / len(pieces), top_value / len(pieces))
        return jnp.repeat(jnp.exp(draws), shape[position] // blocks).reshape((-1,) + (1,) * (len(shape) - position - 1))

    gain = one(*pieces[0])
    for cut in pieces[1:]:
        gain = gain * one(*cut)
    return gain


def normal_values(own_key, extent, spread, bound, pieces=(), held_as=jnp.bfloat16):
    loudness = shard_levels(own_key, extent, pieces, -0.22, 0.18) if pieces else 1.0
    result = jax.random.normal(own_key, extent, jnp.float32) * spread * loudness
    return jnp.minimum(jnp.maximum(result, -bound), bound).astype(held_as)


def setup_inputs(seed: int = 0) -> dict:
    key_of = jax.random.split(jax.random.key(seed), 8)
    return {
        "visit_flux": normal_values(key_of[0], (EPOCHS, BLENDS, BANDS, PIX), 1.0, 6.0, ((0, 4), (3, 8))),
        "visit_precision": jnp.clip(jnp.exp(math.log(4.0) - 2.7725887 * jax.random.uniform(key_of[1], (EPOCHS, BLENDS, BANDS, PIX), jnp.float32) ** shard_levels(key_of[1], (EPOCHS, BLENDS, BANDS, PIX), ((0, 4), (3, 8)), -0.2, 0.2)), 0.25, 4.0).astype(jnp.bfloat16),
        "visit_live": with_ends((jax.random.randint(key_of[2], (EPOCHS, BLENDS), 0, 4) < 3).astype(jnp.int32), jax.random.fold_in(key_of[2], 1), 0, 1),
        "footprint": with_ends((jax.random.randint(key_of[3], (BLENDS, SRC, PIX), 0, 2) < 1).astype(jnp.int32), jax.random.fold_in(key_of[3], 1), 0, 1),
        "source_count": with_ends(jax.random.randint(key_of[4], (BLENDS,), 1, SRC + 1), jax.random.fold_in(key_of[4], 1), 1, SRC).astype(jnp.int32),
        "spectra_init": jnp.clip(0.2 + 1 * jax.random.uniform(key_of[5], (BLENDS, SRC, BANDS), jnp.float32) ** shard_levels(key_of[5], (BLENDS, SRC, BANDS), ((0, 8),), -0.2, 0.2), 0.2, 1.2),
        "morphology_init": jnp.clip(0.25 * jax.random.uniform(key_of[6], (BLENDS, SRC, PIX), jnp.float32) ** shard_levels(key_of[6], (BLENDS, SRC, PIX), ((0, 8), (2, 4)), -0.2, 0.2), 0.0, 0.25),
    }


def reference(visit_flux, visit_precision, visit_live, footprint, source_count, spectra_init, morphology_init):
    def accumulate(totals, visit):
        flux_one, precision_one, live_one = visit
        weights = precision_one.astype(jnp.float32) * live_one.astype(jnp.float32)[:, None, None]
        return (totals[0] + weights * flux_one.astype(jnp.float32), totals[1] + weights), None

    zeros = jnp.zeros(visit_flux.shape[1:], jnp.float32)
    (numerator, weight_sum), _ = lax.scan(accumulate, (zeros, zeros), (visit_flux, visit_precision, visit_live))
    coadd_flux = numerator / (1.0 + weight_sum)
    coverage = weight_sum / (1.0 + weight_sum)
    source_live = (jnp.arange(SRC, dtype=jnp.int32)[None, :] < source_count[:, None]).astype(jnp.float32)
    footprint_mask = footprint.astype(jnp.float32) * source_live[:, :, None]
    live_count = source_count.astype(jnp.float32)
    morphology = morphology_init * footprint_mask
    spectra = spectra_init
    highest = lax.Precision.HIGHEST
    for iteration in range(ITERS):
        blend_model = jnp.einsum("bkc,bkp->bcp", spectra, morphology, precision=highest)
        residual = coverage * (coadd_flux - blend_model)
        morph_grad = jnp.einsum("bkc,bcp->bkp", spectra, residual, precision=highest)
        morph_step = 1.0 / (1.0 + live_count[:, None] * jnp.sum(spectra * spectra, axis=2))
        morphology = jnp.maximum(0.0, morphology + morph_grad * morph_step[:, :, None]) * footprint_mask
        blend_model = jnp.einsum("bkc,bkp->bcp", spectra, morphology, precision=highest)
        residual = coverage * (coadd_flux - blend_model)
        spectra_grad = jnp.einsum("bkp,bcp->bkc", morphology, residual, precision=highest)
        morph_norm = jnp.sum(morphology * morphology, axis=2)
        spectra = jnp.maximum(0.0, spectra + spectra_grad / (1.0 + live_count[:, None] * morph_norm)[:, :, None])
    return coadd_flux, spectra, morphology
```

```python
import functools

import jax
import jax.numpy as jnp
from jax import lax
from jax.experimental import pallas as pl
from jax.experimental.pallas import tpu as pltpu
from jax.sharding import PartitionSpec as P

ITERS = 2


LANES = 128
MESH = pl.DeviceIdType.MESH
AHEAD = 3
LAG = 2


def factors(count):
    rows = max(d for d in range(1, count + 1) if count % d == 0 and d * d <= count)
    return rows, count // rows


def cut(chunks, bands):
    half = max(1, bands // 2)
    return [
        (q, lo, min(bands, lo + half)) for q in range(chunks) for lo in range(0, bands, half)
    ]


def bits(count):
    return [1 << k for k in range(count.bit_length() - 1)]


def flip(at, bit):
    return at + bit - 2 * bit * (at // bit % 2)


def coadd_kernel(
    flux_hbm, prec_hbm, live_hbm, foot_hbm, count_hbm, spec_hbm, morph_hbm,
    coadd_ref, spec_out, morph_ref,
    in_v, live_ref, foot_v, count_ref, spec_ref, flux_c, cover,
    stage, land1, part, land2, final, pieces, spectra, step_ref, acc, sums,
    in_sem, side_sem, near_sem, send_sem, s1_recv, s2_recv, s3_recv, ps_recv,
    *, ne, nb,
):
    visits, bands, every_blend, block = flux_hbm.shape
    owned, slots, pix_part = morph_hbm.shape
    chunks = in_v.shape[1]
    width = block // chunks
    per_dest = pix_part // block
    held = per_dest * owned
    e = lax.axis_index("epoch")
    j = lax.axis_index("blend")
    y, x = e // 2, e % 2
    home_e = j // per_dest
    home_slot = j % per_dest
    f32 = jnp.float32
    work = cut(chunks, bands)
    count_of = len(work)
    loads = [w for w in work if w[0] == 0] + [(q, 0, bands) for q in range(1, chunks)]

    small = [
        pltpu.make_async_copy(src, dst, side_sem.at[k])
        for k, (src, dst) in enumerate(
            ((live_hbm, live_ref), (count_hbm, count_ref), (spec_hbm, spec_ref)))
    ]
    small[0].start()

    def in_copy(n):
        q, lo, hi = loads[n]
        window, some = pl.ds(q * width, width), pl.ds(lo, hi - lo)
        return [
            pltpu.make_async_copy(
                src.at[:, some, :, window], in_v.at[k, q, :, some], in_sem.at[n])
            for k, src in enumerate((prec_hbm, flux_hbm))
        ]

    def in_wait(n):
        q, lo, hi = loads[n]
        here = in_v.at[:, q, :, pl.ds(lo, hi - lo)]
        pltpu.make_async_copy(here, here, in_sem.at[n]).wait()

    for n in range(len(loads)):
        for copy in in_copy(n):
            copy.start()

    near = [(flip(e, bit), j) for bit in bits(ne)] + [(e, flip(j, bit)) for bit in bits(nb)]
    barrier = pltpu.get_barrier_semaphore()
    for other in near:
        pl.semaphore_signal(barrier, inc=1, device_id=other, device_id_type=MESH)

    def spread(k):
        if k > 1:
            pl.semaphore_wait(near_sem.at[k - 2], 1)
        if k < len(near):
            pl.semaphore_signal(
                near_sem.at[k - 1], inc=1, device_id=near[k], device_id_type=MESH)

    for copy in small[1:]:
        copy.start()
    side = []
    for s in range(per_dest):
        for b in range(owned):
            row = s * owned + b
            window = pl.ds(s * block, block)
            side.append(pltpu.make_async_copy(
                foot_hbm.at[b, :, window], foot_v.at[:, row, :], side_sem.at[3]))
            side.append(pltpu.make_async_copy(
                morph_hbm.at[b, :, window], morph_ref.at[:, row, :], side_sem.at[4]))

    small[0].wait()
    square_r = lax.broadcasted_iota(jnp.int32, (every_blend, every_blend), 0)
    square_c = lax.broadcasted_iota(jnp.int32, (every_blend, every_blend), 1)
    lives = []
    for v in range(visits):
        row = jnp.broadcast_to(live_ref[v : v + 1, :].astype(f32), (every_blend, every_blend))
        column = jnp.sum(jnp.where(square_r == square_c, row, 0.0), axis=1, keepdims=True)
        lives.append(jnp.broadcast_to(column, (every_blend, LANES)))

    def local_sum(i):
        q, lo, hi = work[i]
        for n, (r, start, _) in enumerate(loads):
            if r == q and start == lo:
                in_wait(n)

        def one(c, carry):
            for p in range(ne):
                lanes = slice(p * LANES, (p + 1) * LANES)
                py, px = p // 2, p % 2
                num = None
                for v in range(visits):
                    w = in_v[0, q, v, c, :, lanes].astype(f32) * lives[v]
                    n = w * in_v[1, q, v, c, :, lanes].astype(f32)
                    num, wsum = (n, w) if num is None else (num + n, wsum + w)
                stage[0, q, px * 2 + py, c] = num
                stage[1, q, py * 2 + px, c] = wsum
            return carry

        lax.fori_loop(lo, hi, one, 0)

    along = (x, y)
    across = (y, x)
    mate = (near[0], near[1])

    def s1(a, i):
        q, lo, hi = work[i]
        some = pl.ds(lo, hi - lo)
        return pltpu.make_async_remote_copy(
            src_ref=stage.at[a, q, pl.ds((1 - along[a]) * 2, 2), some],
            dst_ref=land1.at[a, q, :, some],
            send_sem=send_sem.at[0], recv_sem=s1_recv.at[i],
            device_id=mate[a], device_id_type=MESH,
        )

    def s2(a, i):
        q, lo, hi = work[i]
        some = pl.ds(lo, hi - lo)
        return pltpu.make_async_remote_copy(
            src_ref=part.at[a, q, 1 - across[a], some],
            dst_ref=land2.at[a, q, some],
            send_sem=send_sem.at[1], recv_sem=s2_recv.at[i],
            device_id=mate[1 - a], device_id_type=MESH,
        )

    def s1_start(i):
        for a in range(2):
            s1(a, i).start()

    def s2_start(i):
        q, lo, hi = work[i]
        here = land1.at[:, q, :, pl.ds(lo, hi - lo)]
        pltpu.make_async_copy(here, here, s1_recv.at[i]).wait()

        def add(c, carry):
            for a in range(2):
                for o in range(2):
                    part[a, q, o, c] = stage[a, q, along[a] * 2 + o, c] + land1[a, q, o, c]
            return carry

        lax.fori_loop(lo, hi, add, 0)
        for a in range(2):
            s2(a, i).start()

    here = home_e == e

    def landing(i):
        q, lo, hi = work[i]
        lanes = pl.ds(pl.multiple_of(e * LANES, LANES), LANES)
        return pieces.at[q, :, pl.ds(lo, hi - lo), home_slot, :, lanes]

    def leaving(i, to):
        q, lo, hi = work[i]
        return final.at[q, to, :, pl.ds(lo, hi - lo)]

    def s3_local(i):
        return pltpu.make_async_copy(leaving(i, j), landing(i), s3_recv.at[work[i][0]])

    def s3_remote(i, to):
        return pltpu.make_async_remote_copy(
            src_ref=leaving(i, to), dst_ref=landing(i),
            send_sem=send_sem.at[2], recv_sem=s3_recv.at[work[i][0]],
            device_id=(home_e, to), device_id_type=MESH,
        )

    def s3_start(i):
        q, lo, hi = work[i]
        there = land2.at[:, q, pl.ds(lo, hi - lo)]
        pltpu.make_async_copy(there, there, s2_recv.at[i]).wait()

        def add(c, carry):
            for a in range(2):
                v = part[a, q, across[a], c] + land2[a, q, c]
                for to in range(nb):
                    final[q, to, a, c] = v[to * owned : (to + 1) * owned, :]
            return carry

        lax.fori_loop(lo, hi, add, 0)

        def send(d, carry):
            s3_remote(i, lax.rem(j + d, nb)).start()
            return carry

        lax.fori_loop(1, nb, send, 0)

        @pl.when(here)
        def _():
            s3_local(i).start()

        @pl.when(jnp.logical_not(here))
        def _():
            s3_remote(i, j).start()

    sub = lax.broadcasted_iota(jnp.int32, (held, LANES), 0)
    lane = lax.broadcasted_iota(jnp.int32, (held, LANES), 1)
    state = []

    def steps():
        for k in range(slots):
            norm = None
            for c in range(bands):
                s = spectra[k, c]
                norm = s * s if norm is None else norm + s * s
            step_ref[k] = 1.0 / (1.0 + state[1] * norm)

    group = 2

    def deblend(start, first):
        runs = [
            pl.ds(pl.multiple_of(start + t * LANES, LANES), LANES) for t in range(group)
        ]

        def masks(k):
            live = jnp.where(state[0] > k, 1.0, 0.0).astype(f32)
            return [foot_v[k, :, px].astype(f32) * live for px in runs]

        def residual(morph):
            res = []
            for c in range(bands):
                model = [None] * group
                for k in range(slots):
                    s = spectra[k, c]
                    for t in range(group):
                        v = s * morph[k][t]
                        model[t] = v if k == 0 else model[t] + v
                res.append([
                    cover[c, :, px] * (flux_c[c, :, px] - model[t]) for t, px in enumerate(runs)
                ])
            return res

        morph = []
        for k in range(slots):
            m = [morph_ref[k, :, px] for px in runs]
            morph.append([a * b for a, b in zip(m, masks(k))] if first else m)
        res = residual(morph)
        for k in range(slots):
            mask = masks(k)
            grad = [None] * group
            for c in range(bands):
                s = spectra[k, c]
                for t in range(group):
                    v = s * res[c][t]
                    grad[t] = v if c == 0 else grad[t] + v
            step = step_ref[k]
            for t, px in enumerate(runs):
                m = jnp.maximum(0.0, morph[k][t] + grad[t] * step) * mask[t]
                morph[k][t] = m
                morph_ref[k, :, px] = m
        res = residual(morph)
        for k in range(slots):
            for c in range(bands):
                v = acc[k, c]
                for t in range(group):
                    v = v + morph[k][t] * res[c][t]
                acc[k, c] = v
            v = acc[k, bands]
            for t in range(group):
                v = v + morph[k][t] * morph[k][t]
            acc[k, bands] = v

    def finish(q):
        pltpu.make_async_copy(pieces.at[q], pieces.at[q], s3_recv.at[q]).wait()
        at = slice(q * width, (q + 1) * width)

        def unpack(c, carry):
            for s in range(per_dest):
                rows = slice(s * owned, (s + 1) * owned)
                wsum = pieces[q, 1, c, s]
                inv = 1.0 / (1.0 + wsum)
                flux = pieces[q, 0, c, s] * inv
                coadd_ref[c, :, s * block + q * width : s * block + (q + 1) * width] = flux
                flux_c[c, rows, at] = flux
                cover[c, rows, at] = wsum * inv
            return carry

        lax.fori_loop(0, bands, unpack, 0)

        def go(i, carry):
            deblend(q * width + i * (group * LANES), True)
            return carry

        lax.fori_loop(0, width // (group * LANES), go, 0)

    def ps_copy(it, d):
        to = lax.rem(e + d, ne)
        return pltpu.make_async_remote_copy(
            src_ref=sums.at[it, 0], dst_ref=sums.at[it, d],
            send_sem=send_sem.at[3], recv_sem=ps_recv.at[it],
            device_id=(to, j), device_id_type=MESH,
        )

    def drain():
        pltpu.make_async_copy(land1, land1, send_sem.at[0]).wait()
        pltpu.make_async_copy(land2, land2, send_sem.at[1]).wait()

        @pl.when(here)
        def _():
            some = final.at[:, pl.ds(0, nb - 1)]
            pltpu.make_async_copy(some, some, send_sem.at[2]).wait()

        @pl.when(jnp.logical_not(here))
        def _():
            pltpu.make_async_copy(final, final, send_sem.at[2]).wait()

    def update(it):
        packed = jnp.zeros((held, LANES), f32)
        for k in range(slots):
            for c in range(bands + 1):
                whole = jnp.sum(acc[k, c], axis=1, keepdims=True)
                packed = jnp.where(lane == k * (bands + 1) + c, whole, packed)
        sums[it, 0] = packed
        for d in range(1, ne):
            ps_copy(it, d).start()
        if it == ITERS - 1:
            drain()
        arrived = sums.at[it, pl.ds(1, ne - 1)]
        pltpu.make_async_copy(arrived, arrived, ps_recv.at[it]).wait()
        whole = None
        for o in range(ne):
            v = sums[it, lax.rem(e - o + ne, ne)]
            whole = v if whole is None else whole + v
        one = whole[0:owned, :]
        for s in range(1, per_dest):
            one = one + whole[s * owned : (s + 1) * owned, :]
        whole = jnp.concatenate([one] * per_dest, axis=0)
        for k in range(slots):
            at = k * (bands + 1)
            norm = jnp.broadcast_to(whole[:, at + bands : at + bands + 1], (held, LANES))
            scale = 1.0 / (1.0 + state[1] * norm)
            for c in range(bands):
                grad = jnp.broadcast_to(whole[:, at + c : at + c + 1], (held, LANES))
                spectra[k, c] = jnp.maximum(0.0, spectra[k, c] + grad * scale)

    local_sum(0)
    pl.semaphore_wait(barrier, len(near))
    s1_start(0)
    spread(1)
    for i in range(1, min(AHEAD, count_of)):
        local_sum(i)
        s1_start(i)
        spread(i + 1)
    for copy in side:
        copy.start()

    for copy in small[1:]:
        copy.wait()
    count = jnp.zeros((held, LANES), jnp.int32)
    for b in range(owned):
        count = jnp.where(lax.rem(sub, owned) == b, count_ref[b], count)
    state.extend((count, count.astype(f32)))
    acc[...] = jnp.zeros_like(acc)
    for k in range(slots):
        for c in range(bands):
            start = jnp.broadcast_to(spec_ref[c, :, k : k + 1], (owned, LANES))
            spectra[k, c] = jnp.concatenate([start] * per_dest, axis=0)
    steps()

    for k in range(min(AHEAD, count_of) + 1, len(near)):
        spread(k)
    for i in range(count_of + LAG):
        if i < count_of:
            s2_start(i)
        if i + AHEAD < count_of:
            local_sum(i + AHEAD)
            s1_start(i + AHEAD)
        if i == LAG:
            spread(len(near))
        if 0 <= i - LAG < count_of:
            s3_start(i - LAG)
    for done, copies in ((foot_v, 3), (morph_ref, 4)):
        pltpu.make_async_copy(done, done, side_sem.at[copies]).wait()
    for q in range(chunks):
        finish(q)

    update(0)
    for it in range(1, ITERS):
        steps()
        acc[...] = jnp.zeros_like(acc)

        def again(i, carry):
            deblend(i * (group * LANES), False)
            return carry

        lax.fori_loop(0, block // (group * LANES), again, 0)
        update(it)
    for c in range(bands):
        out = spectra[0, c]
        for k in range(1, slots):
            out = jnp.where(lane == k, spectra[k, c], out)
        spec_out[c] = out[0:owned, :slots]

    gone = sums.at[:, pl.ds(1, ne - 1)]
    pltpu.make_async_copy(gone, gone, send_sem.at[3]).wait()


def hand_over(coadd_in, spec_in, morph_in, coadd_out, spec_out, morph_out, sems):
    owned, _, pix_part = morph_out.shape
    _, held, block = morph_in.shape
    for row in range(held):
        pltpu.make_async_copy(
            morph_in.at[:, row, :],
            morph_out.at[row % owned, :, pl.ds(row // owned * block, block)], sems.at[2]).start()
    others = [pltpu.make_async_copy(coadd_in, coadd_out, sems.at[0]),
              pltpu.make_async_copy(spec_in, spec_out, sems.at[1])]
    for copy in others:
        copy.start()
    pltpu.make_async_copy(morph_in, morph_in, sems.at[2]).wait()
    for copy in others:
        copy.wait()


def fused(ne, nb, visit_flux, visit_precision, visit_live, footprint, source_count, spectra_init,
          morphology_init):
    visits, every_blend, bands, block = visit_flux.shape
    owned, slots, pix_part = morphology_init.shape
    width = ne * LANES
    chunks = block // width
    per_dest = pix_part // block
    held = per_dest * owned
    count_of = len(cut(chunks, bands))
    loads = count_of // chunks + chunks - 1
    f32 = jnp.float32
    vmem, hbm = (pl.BlockSpec(memory_space=s) for s in (pltpu.VMEM, pl.ANY))
    dma = pltpu.SemaphoreType.DMA
    parts = pl.pallas_call(
        functools.partial(coadd_kernel, ne=ne, nb=nb),
        out_shape=(
            pltpu.VMEM((bands, owned, pix_part), f32),
            pltpu.VMEM((bands, owned, slots), f32),
            pltpu.VMEM((slots, held, block), f32),
        ),
        in_specs=[hbm] * 7,
        out_specs=(vmem, vmem, vmem),
        scratch_shapes=[
            pltpu.VMEM((2, chunks, visits, bands, every_blend, width), visit_flux.dtype),
            pltpu.VMEM(visit_live.shape, jnp.int32),
            pltpu.VMEM((slots, held, block), jnp.int32),
            pltpu.SMEM(source_count.shape, jnp.int32),
            pltpu.VMEM((bands, owned, slots), f32),
            pltpu.VMEM((bands, held, block), f32),
            pltpu.VMEM((bands, held, block), f32),
            pltpu.VMEM((2, chunks, ne, bands, every_blend, LANES), f32),
            pltpu.VMEM((2, chunks, 2, bands, every_blend, LANES), f32),
            pltpu.VMEM((2, chunks, 2, bands, every_blend, LANES), f32),
            pltpu.VMEM((2, chunks, bands, every_blend, LANES), f32),
            pltpu.VMEM((chunks, nb, 2, bands, owned, LANES), f32),
            pltpu.VMEM((chunks, 2, bands, per_dest, owned, width), f32),
            pltpu.VMEM((slots, bands, held, LANES), f32),
            pltpu.VMEM((slots, held, LANES), f32),
            pltpu.VMEM((slots, bands + 1, held, LANES), f32),
            pltpu.VMEM((ITERS, ne, held, LANES), f32),
            dma((loads,)),
            dma((5,)),
            pltpu.SemaphoreType.REGULAR((len(bits(ne)) + len(bits(nb)) - 1,)),
            dma((4,)),
            dma((count_of,)),
            dma((count_of,)),
            dma((chunks,)),
            dma((ITERS,)),
        ],
        compiler_params=pltpu.CompilerParams(
            collective_id=0, has_side_effects=True, vmem_limit_bytes=58 * 2**20
        ),
    )(visit_flux.transpose(0, 2, 1, 3), visit_precision.transpose(0, 2, 1, 3), visit_live,
      footprint, source_count, spectra_init.transpose(2, 0, 1), morphology_init)
    coadd, spectra, morphology = pl.pallas_call(
        hand_over,
        out_shape=(
            jax.ShapeDtypeStruct((bands, owned, pix_part), f32),
            jax.ShapeDtypeStruct((bands, owned, slots), f32),
            jax.ShapeDtypeStruct((owned, slots, pix_part), f32),
        ),
        in_specs=[vmem] * 3,
        out_specs=(hbm,) * 3,
        scratch_shapes=[dma((3,))],
        compiler_params=pltpu.CompilerParams(vmem_limit_bytes=8 * 2**20),
    )(*parts)
    return coadd.transpose(1, 0, 2), spectra.transpose(1, 2, 0), morphology


def on_device(
    visit_flux, visit_precision, visit_live, footprint, source_count, spectra_init, morphology_init
):
    weights = visit_precision.astype(jnp.float32) * visit_live.astype(jnp.float32)[:, :, None, None]
    numerator = jnp.sum(weights * visit_flux.astype(jnp.float32), axis=0)
    weight_sum = jnp.sum(weights, axis=0)
    pix_part = morphology_init.shape[2]
    owned = morphology_init.shape[0]
    numerator, weight_sum = (
        lax.psum_scatter(numerator, "epoch", scatter_dimension=2, tiled=True),
        lax.psum_scatter(weight_sum, "epoch", scatter_dimension=2, tiled=True),
    )
    every_blend, band_count, piece = numerator.shape
    numerator = numerator.reshape(every_blend, band_count, 1, piece)
    weight_sum = weight_sum.reshape(every_blend, band_count, 1, piece)
    numerator, weight_sum = (
        lax.all_to_all(numerator, "blend", split_axis=0, concat_axis=2, tiled=True),
        lax.all_to_all(weight_sum, "blend", split_axis=0, concat_axis=2, tiled=True),
    )
    blocks = numerator.shape[2]
    numerator = numerator.reshape(owned, band_count, blocks, 1, piece)
    weight_sum = weight_sum.reshape(owned, band_count, blocks, 1, piece)
    numerator, weight_sum = (
        lax.all_to_all(numerator, "epoch", split_axis=2, concat_axis=3, tiled=True),
        lax.all_to_all(weight_sum, "epoch", split_axis=2, concat_axis=3, tiled=True),
    )
    numerator = numerator.reshape(owned, band_count, pix_part)
    weight_sum = weight_sum.reshape(owned, band_count, pix_part)
    coadd_flux = numerator / (1.0 + weight_sum)
    coverage = weight_sum / (1.0 + weight_sum)
    slots = footprint.shape[1]
    source_live = (jnp.arange(slots, dtype=jnp.int32)[None, :] < source_count[:, None]).astype(
        jnp.float32
    )
    footprint_mask = footprint.astype(jnp.float32) * source_live[:, :, None]
    live_count = source_count.astype(jnp.float32)
    morphology = morphology_init * footprint_mask
    spectra = spectra_init
    highest = lax.Precision.HIGHEST
    for iteration in range(ITERS):
        blend_model = jnp.einsum("bkc,bkp->bcp", spectra, morphology, precision=highest)
        residual = coverage * (coadd_flux - blend_model)
        morph_grad = jnp.einsum("bkc,bcp->bkp", spectra, residual, precision=highest)
        morph_step = 1.0 / (1.0 + live_count[:, None] * jnp.sum(spectra * spectra, axis=2))
        morphology = (
            jnp.maximum(0.0, morphology + morph_grad * morph_step[:, :, None]) * footprint_mask
        )
        blend_model = jnp.einsum("bkc,bkp->bcp", spectra, morphology, precision=highest)
        residual = coverage * (coadd_flux - blend_model)
        spectra_grad = jnp.einsum("bkp,bcp->bkc", morphology, residual, precision=highest)
        morph_norm = jnp.sum(morphology * morphology, axis=2)
        spectra_grad, morph_norm = lax.psum((spectra_grad, morph_norm), "epoch")
        spectra = jnp.maximum(
            0.0, spectra + spectra_grad / (1.0 + live_count[:, None] * morph_norm)[:, :, None]
        )
    return (coadd_flux, spectra, morphology)


def solution(mesh):
    ne, nb = mesh.shape["epoch"], mesh.shape["blend"]

    def step(visit_flux, visit_precision, visit_live, footprint, source_count, spectra_init,
             morphology_init):
        block, bands = visit_flux.shape[3], visit_flux.shape[2]
        owned, pix_part = morphology_init.shape[0], morphology_init.shape[2]
        fits = (
            block % (ne * LANES) == 0
            and pix_part % block == 0
            and factors(ne) == (2, 2)
            and nb & (nb - 1) == 0
            and AHEAD <= block // (ne * LANES) * bands
            and morphology_init.shape[1] * (bands + 1) <= LANES
        )
        run = functools.partial(fused, ne, nb) if fits else on_device
        return run(visit_flux, visit_precision, visit_live, footprint, source_count, spectra_init,
                   morphology_init)

    in_specs = (
        P("epoch", None, None, "blend"),
        P("epoch", None, None, "blend"),
        P("epoch", None),
        P("blend", None, "epoch"),
        P("blend"),
        P("blend", None, None),
        P("blend", None, "epoch"),
    )
    out_specs = (P("blend", None, "epoch"), P("blend", None, None), P("blend", None, "epoch"))
    return jax.shard_map(
        step, mesh=mesh, in_specs=in_specs, out_specs=out_specs, check_vma=False
    )
```

```python
import functools

import jax
import jax.numpy as jnp
from jax import lax
from jax.experimental import pallas as pl
from jax.experimental.pallas import tpu as pltpu
from jax.sharding import PartitionSpec as P

ITERS = 2


LANES = 128
MESH = pl.DeviceIdType.MESH
CUTS = 3
AHEAD = 4
LAG = 3
ROUTES = (
    (0, 0, 1, 6), (0, 2, 1, 2),
    (1, 0, 0, 3), (1, 1, 0, 5),
    (2, 0, 0, 4), (2, 2, 1, 2), (2, 3, 1, 2),
    (3, 1, 0, 4), (3, 2, 1, 4),
)


def factors(count):
    rows = max(d for d in range(1, count + 1) if count % d == 0 and d * d <= count)
    return rows, count // rows


def cut(chunks, bands):
    step = max(1, bands // CUTS)
    return [
        (q, lo, min(bands, lo + step)) for q in range(chunks) for lo in range(0, bands, step)
    ]


def plan():
    unit, runs = {}, []
    for t, p, first, n in ROUTES:
        runs.append((first, p >> first & 1, p >> 1 - first & 1, t, p, unit.get(t, 0), n))
        unit[t] = unit.get(t, 0) + n
    slot, placed = 0, []
    for first, one, two, t, p, u, n in sorted(runs):
        placed.append((first, one, two, t, p, u, n, slot))
        slot += n
    return placed, slot


def span(runs):
    runs = list(runs)
    return (min(r[7] for r in runs), sum(r[6] for r in runs)) if runs else (0, 0)


def slots_of(runs):
    return [r[7] + k for r in runs for k in range(r[6])]


def bits(count):
    return [1 << k for k in range(count.bit_length() - 1)]


def flip(at, bit):
    return at + bit - 2 * bit * (at // bit % 2)


def coadd_kernel(
    flux_hbm, prec_hbm, live_hbm, foot_hbm, count_hbm, spec_hbm, morph_hbm,
    coadd_ref, spec_out, morph_ref,
    in_v, live_ref, foot_v, count_ref, spec_ref, flux_c, cover,
    stage, land1, land2, final, pieces, spectra, step_ref, acc, sums,
    in_sem, side_sem, near_sem, send_sem, s1_recv, s2_recv, s3_recv, ps_recv,
    *, ne, nb,
):
    visits, bands, every_blend, block = flux_hbm.shape
    owned, slots, pix_part = morph_hbm.shape
    chunks = in_v.shape[1]
    width = block // chunks
    per_dest = pix_part // block
    held = per_dest * owned
    e = lax.axis_index("epoch")
    j = lax.axis_index("blend")
    y, x = e // 2, e % 2
    home_e = j // per_dest
    home_slot = j % per_dest
    f32 = jnp.float32
    work = cut(chunks, bands)
    runs, slot_count = plan()
    place = (x + home_e) % 2 + (y + home_e // 2) % 2 * 2
    slot_at = []
    for to in range(ne):
        b0, b1 = (home_e + to) % 2, (home_e // 2 + to // 2) % 2
        spots = []
        for u in range(2 * ne):
            t0, t1, t2, t3 = (
                next(r[7] + u - r[5] for r in runs if r[3] == t and r[5] <= u < r[5] + r[6])
                for t in range(ne)
            )
            spots.append(t0 + b0 * (t1 - t0) + b1 * (t2 - t0) + b0 * b1 * (t3 - t2 - t1 + t0))
        slot_at.append(spots)
    count_of = len(work)
    loads = [w for w in work if w[0] == 0] + [(q, 0, bands) for q in range(1, chunks)]

    small = [
        pltpu.make_async_copy(src, dst, side_sem.at[k])
        for k, (src, dst) in enumerate(
            ((live_hbm, live_ref), (count_hbm, count_ref), (spec_hbm, spec_ref)))
    ]
    small[0].start()

    def in_copy(n):
        q, lo, hi = loads[n]
        window, some = pl.ds(q * width, width), pl.ds(lo, hi - lo)
        return [
            pltpu.make_async_copy(
                src.at[:, some, :, window], in_v.at[k, q, :, some], in_sem.at[n])
            for k, src in enumerate((prec_hbm, flux_hbm))
        ]

    def in_wait(n):
        q, lo, hi = loads[n]
        here = in_v.at[:, q, :, pl.ds(lo, hi - lo)]
        pltpu.make_async_copy(here, here, in_sem.at[n]).wait()

    for n in range(len(loads)):
        for copy in in_copy(n):
            copy.start()

    near = [(flip(e, bit), j) for bit in bits(ne)] + [(e, flip(j, bit)) for bit in bits(nb)]
    barrier = pltpu.get_barrier_semaphore()
    for other in near:
        pl.semaphore_signal(barrier, inc=1, device_id=other, device_id_type=MESH)

    def spread(k):
        if k > 1:
            pl.semaphore_wait(near_sem.at[k - 2], 1)
        if k < len(near):
            pl.semaphore_signal(
                near_sem.at[k - 1], inc=1, device_id=near[k], device_id_type=MESH)

    for copy in small[1:]:
        copy.start()
    side = []
    for s in range(per_dest):
        for b in range(owned):
            row = s * owned + b
            window = pl.ds(s * block, block)
            side.append(pltpu.make_async_copy(
                foot_hbm.at[b, :, window], foot_v.at[:, row, :], side_sem.at[3]))
            side.append(pltpu.make_async_copy(
                morph_hbm.at[b, :, window], morph_ref.at[:, row, :], side_sem.at[4]))

    small[0].wait()
    square_r = lax.broadcasted_iota(jnp.int32, (every_blend, every_blend), 0)
    square_c = lax.broadcasted_iota(jnp.int32, (every_blend, every_blend), 1)
    lives = []
    for v in range(visits):
        row = jnp.broadcast_to(live_ref[v : v + 1, :].astype(f32), (every_blend, every_blend))
        column = jnp.sum(jnp.where(square_r == square_c, row, 0.0), axis=1, keepdims=True)
        lives.append(jnp.broadcast_to(column, (every_blend, LANES)))

    def local_sum(i):
        q, lo, hi = work[i]
        for n, (r, start, _) in enumerate(loads):
            if r == q and start == lo:
                in_wait(n)

        def one(c, carry):
            for g in range(ne):
                lanes = slice(g * LANES, (g + 1) * LANES)
                num = None
                for v in range(visits):
                    w = in_v[0, q, v, c, :, lanes].astype(f32) * lives[v]
                    n = w * in_v[1, q, v, c, :, lanes].astype(f32)
                    num, wsum = (n, w) if num is None else (num + n, wsum + w)
                for k, total in enumerate((num, wsum)):
                    for to in range(ne):
                        stage[q, slot_at[to][k * ne + g], c] = total[to * held : (to + 1) * held, :]
            return carry

        lax.fori_loop(lo, hi, one, 0)

    def at_place(act):
        for p in range(ne):
            @pl.when(place == p)
            def _(p=p):
                act(p)

    def kept(p, first):
        return [r for r in runs if r[0] == first and r[1] == p >> first & 1]

    def given(p, first):
        return [r for r in runs if r[0] == first and r[1] != p >> first & 1]

    def passed(p, first):
        return [r for r in kept(p, first) if r[2] != p >> 1 - first & 1]

    def owned_at(p):
        return [r for r in runs if r[4] == p]

    def exchange(src, dst, i, sent, to, send, recv):
        q, lo, hi = work[i]
        first, n = span(sent)
        if n:
            piece = (q, pl.ds(first, n), pl.ds(lo, hi - lo))
            pltpu.make_async_remote_copy(
                src_ref=src.at[piece], dst_ref=dst.at[piece],
                send_sem=send_sem.at[send], recv_sem=recv.at[i],
                device_id=to, device_id_type=MESH,
            ).start()

    def arrive(ref, i, n, recv):
        q, lo, hi = work[i]
        if n:
            here = ref.at[q, pl.ds(0, n), pl.ds(lo, hi - lo)]
            pltpu.make_async_copy(here, here, recv.at[i]).wait()

    def s1_start(i):
        def act(p):
            for first in range(2):
                exchange(stage, land1, i, given(p, first), near[first], 0, s1_recv)

        at_place(act)

    def s2_start(i):
        q, lo, hi = work[i]

        def act(p):
            mine = slots_of(kept(p, 0) + kept(p, 1))
            arrive(land1, i, len(mine), s1_recv)

            def add(c, carry):
                for k in mine:
                    stage[q, k, c] = stage[q, k, c] + land1[q, k, c]
                return carry

            lax.fori_loop(lo, hi, add, 0)
            for first in range(2):
                exchange(stage, land2, i, passed(p, first), near[1 - first], 1, s2_recv)

        at_place(act)

    def s3_start(i):
        q, lo, hi = work[i]
        some = pl.ds(lo, hi - lo)

        def act(p):
            mine = slots_of(owned_at(p))
            arrive(land2, i, len(mine), s2_recv)

            def add(c, carry):
                for k in mine:
                    v = stage[q, k, c] + land2[q, k, c]
                    for to in range(per_dest):
                        final[q, to, k, c] = v[to * owned : (to + 1) * owned, :]
                return carry

            lax.fori_loop(lo, hi, add, 0)
            for _, _, _, t, _, u, n, first in owned_at(p):
                over = j
                for bit in bits(ne):
                    if t & bit:
                        over = flip(over, bit * per_dest)
                for d in (1, 0):
                    to = flip(over, 1) if d else over
                    src = final.at[q, to % per_dest, pl.ds(first, n), some]
                    dst = pieces.at[q, home_slot, pl.ds(u, n), some]
                    if p == 0 and t == 0 and d == 0:
                        pltpu.make_async_copy(src, dst, s3_recv.at[q]).start()
                    else:
                        pltpu.make_async_remote_copy(
                            src_ref=src, dst_ref=dst,
                            send_sem=send_sem.at[2], recv_sem=s3_recv.at[q],
                            device_id=(home_e, to), device_id_type=MESH,
                        ).start()

        at_place(act)

    sub = lax.broadcasted_iota(jnp.int32, (held, LANES), 0)
    lane = lax.broadcasted_iota(jnp.int32, (held, LANES), 1)
    state = []

    def steps():
        for k in range(slots):
            norm = None
            for c in range(bands):
                s = spectra[k, c]
                norm = s * s if norm is None else norm + s * s
            step_ref[k] = 1.0 / (1.0 + state[1] * norm)

    group = 2

    def deblend(start, first):
        runs = [
            pl.ds(pl.multiple_of(start + t * LANES, LANES), LANES) for t in range(group)
        ]

        def masks(k):
            live = jnp.where(state[0] > k, 1.0, 0.0).astype(f32)
            return [foot_v[k, :, px].astype(f32) * live for px in runs]

        def residual(morph):
            res = []
            for c in range(bands):
                model = [None] * group
                for k in range(slots):
                    s = spectra[k, c]
                    for t in range(group):
                        v = s * morph[k][t]
                        model[t] = v if k == 0 else model[t] + v
                res.append([
                    cover[c, :, px] * (flux_c[c, :, px] - model[t]) for t, px in enumerate(runs)
                ])
            return res

        morph = []
        for k in range(slots):
            m = [morph_ref[k, :, px] for px in runs]
            morph.append([a * b for a, b in zip(m, masks(k))] if first else m)
        res = residual(morph)
        for k in range(slots):
            mask = masks(k)
            grad = [None] * group
            for c in range(bands):
                s = spectra[k, c]
                for t in range(group):
                    v = s * res[c][t]
                    grad[t] = v if c == 0 else grad[t] + v
            step = step_ref[k]
            for t, px in enumerate(runs):
                m = jnp.maximum(0.0, morph[k][t] + grad[t] * step) * mask[t]
                morph[k][t] = m
                morph_ref[k, :, px] = m
        res = residual(morph)
        for k in range(slots):
            for c in range(bands):
                v = acc[k, c]
                for t in range(group):
                    v = v + morph[k][t] * res[c][t]
                acc[k, c] = v
            v = acc[k, bands]
            for t in range(group):
                v = v + morph[k][t] * morph[k][t]
            acc[k, bands] = v

    def finish(q):
        pltpu.make_async_copy(pieces.at[q], pieces.at[q], s3_recv.at[q]).wait()

        def unpack(c, carry):
            for s in range(per_dest):
                rows = slice(s * owned, (s + 1) * owned)
                for g in range(ne):
                    wsum = pieces[q, s, ne + g, c]
                    inv = 1.0 / (1.0 + wsum)
                    flux = pieces[q, s, g, c] * inv
                    px = q * width + g * LANES
                    coadd_ref[c, :, s * block + px : s * block + px + LANES] = flux
                    flux_c[c, rows, px : px + LANES] = flux
                    cover[c, rows, px : px + LANES] = wsum * inv
            return carry

        lax.fori_loop(0, bands, unpack, 0)

        def go(i, carry):
            deblend(q * width + i * (group * LANES), True)
            return carry

        lax.fori_loop(0, width // (group * LANES), go, 0)

    def ps_copy(it, d):
        to = lax.rem(e + d, ne)
        return pltpu.make_async_remote_copy(
            src_ref=sums.at[it, 0], dst_ref=sums.at[it, d],
            send_sem=send_sem.at[3], recv_sem=ps_recv.at[it],
            device_id=(to, j), device_id_type=MESH,
        )

    def drain():
        def act(p):
            for k, n in enumerate((
                span(given(p, 0))[1] + span(given(p, 1))[1],
                span(passed(p, 0))[1] + span(passed(p, 1))[1],
            )):
                if n:
                    sent = stage.at[:, pl.ds(0, n)]
                    pltpu.make_async_copy(sent, sent, send_sem.at[k]).wait()
            n = sum(r[6] * (per_dest - (p == 0 and r[3] == 0)) for r in owned_at(p))
            sent = final.at[:, 0, pl.ds(0, n)]
            pltpu.make_async_copy(sent, sent, send_sem.at[2]).wait()

        at_place(act)

    def update(it):
        packed = jnp.zeros((held, LANES), f32)
        for k in range(slots):
            for c in range(bands + 1):
                whole = jnp.sum(acc[k, c], axis=1, keepdims=True)
                packed = jnp.where(lane == k * (bands + 1) + c, whole, packed)
        sums[it, 0] = packed
        for d in range(1, ne):
            ps_copy(it, d).start()
        if it == ITERS - 1:
            drain()
        arrived = sums.at[it, pl.ds(1, ne - 1)]
        pltpu.make_async_copy(arrived, arrived, ps_recv.at[it]).wait()
        whole = None
        for o in range(ne):
            v = sums[it, lax.rem(e - o + ne, ne)]
            whole = v if whole is None else whole + v
        one = whole[0:owned, :]
        for s in range(1, per_dest):
            one = one + whole[s * owned : (s + 1) * owned, :]
        whole = jnp.concatenate([one] * per_dest, axis=0)
        for k in range(slots):
            at = k * (bands + 1)
            norm = jnp.broadcast_to(whole[:, at + bands : at + bands + 1], (held, LANES))
            scale = 1.0 / (1.0 + state[1] * norm)
            for c in range(bands):
                grad = jnp.broadcast_to(whole[:, at + c : at + c + 1], (held, LANES))
                spectra[k, c] = jnp.maximum(0.0, spectra[k, c] + grad * scale)

    local_sum(0)
    pl.semaphore_wait(barrier, len(near))
    s1_start(0)
    spread(1)
    for i in range(1, min(AHEAD, count_of)):
        local_sum(i)
        s1_start(i)
        if i + 1 < len(near):
            spread(i + 1)
    for copy in side:
        copy.start()

    for copy in small[1:]:
        copy.wait()
    count = jnp.zeros((held, LANES), jnp.int32)
    for b in range(owned):
        count = jnp.where(lax.rem(sub, owned) == b, count_ref[b], count)
    state.extend((count, count.astype(f32)))
    acc[...] = jnp.zeros_like(acc)
    for k in range(slots):
        for c in range(bands):
            start = jnp.broadcast_to(spec_ref[c, :, k : k + 1], (owned, LANES))
            spectra[k, c] = jnp.concatenate([start] * per_dest, axis=0)
    steps()

    for k in range(min(AHEAD, count_of) + 1, len(near)):
        spread(k)
    for i in range(count_of + LAG):
        if i < count_of:
            s2_start(i)
        if i + AHEAD < count_of:
            local_sum(i + AHEAD)
            s1_start(i + AHEAD)
        if i == LAG:
            spread(len(near))
        if 0 <= i - LAG < count_of:
            s3_start(i - LAG)
    for done, copies in ((foot_v, 3), (morph_ref, 4)):
        pltpu.make_async_copy(done, done, side_sem.at[copies]).wait()
    for q in range(chunks):
        finish(q)

    update(0)
    for it in range(1, ITERS):
        steps()
        acc[...] = jnp.zeros_like(acc)

        def again(i, carry):
            deblend(i * (group * LANES), False)
            return carry

        lax.fori_loop(0, block // (group * LANES), again, 0)
        update(it)
    for c in range(bands):
        out = spectra[0, c]
        for k in range(1, slots):
            out = jnp.where(lane == k, spectra[k, c], out)
        spec_out[c] = out[0:owned, :slots]

    gone = sums.at[:, pl.ds(1, ne - 1)]
    pltpu.make_async_copy(gone, gone, send_sem.at[3]).wait()


def hand_over(coadd_in, spec_in, morph_in, coadd_out, spec_out, morph_out, sems):
    owned, _, pix_part = morph_out.shape
    _, held, block = morph_in.shape
    for row in range(held):
        pltpu.make_async_copy(
            morph_in.at[:, row, :],
            morph_out.at[row % owned, :, pl.ds(row // owned * block, block)], sems.at[2]).start()
    others = [pltpu.make_async_copy(coadd_in, coadd_out, sems.at[0]),
              pltpu.make_async_copy(spec_in, spec_out, sems.at[1])]
    for copy in others:
        copy.start()
    pltpu.make_async_copy(morph_in, morph_in, sems.at[2]).wait()
    for copy in others:
        copy.wait()


def fused(ne, nb, visit_flux, visit_precision, visit_live, footprint, source_count, spectra_init,
          morphology_init):
    visits, every_blend, bands, block = visit_flux.shape
    owned, slots, pix_part = morphology_init.shape
    width = ne * LANES
    chunks = block // width
    per_dest = pix_part // block
    held = per_dest * owned
    count_of = len(cut(chunks, bands))
    loads = count_of // chunks + chunks - 1
    slot_count = plan()[1]
    f32 = jnp.float32
    vmem, hbm = (pl.BlockSpec(memory_space=s) for s in (pltpu.VMEM, pl.ANY))
    dma = pltpu.SemaphoreType.DMA
    parts = pl.pallas_call(
        functools.partial(coadd_kernel, ne=ne, nb=nb),
        out_shape=(
            pltpu.VMEM((bands, owned, pix_part), f32),
            pltpu.VMEM((bands, owned, slots), f32),
            pltpu.VMEM((slots, held, block), f32),
        ),
        in_specs=[hbm] * 7,
        out_specs=(vmem, vmem, vmem),
        scratch_shapes=[
            pltpu.VMEM((2, chunks, visits, bands, every_blend, width), visit_flux.dtype),
            pltpu.VMEM(visit_live.shape, jnp.int32),
            pltpu.VMEM((slots, held, block), jnp.int32),
            pltpu.SMEM(source_count.shape, jnp.int32),
            pltpu.VMEM((bands, owned, slots), f32),
            pltpu.VMEM((bands, held, block), f32),
            pltpu.VMEM((bands, held, block), f32),
            pltpu.VMEM((chunks, slot_count, bands, held, LANES), f32),
            pltpu.VMEM((chunks, slot_count, bands, held, LANES), f32),
            pltpu.VMEM((chunks, slot_count, bands, held, LANES), f32),
            pltpu.VMEM((chunks, per_dest, slot_count, bands, owned, LANES), f32),
            pltpu.VMEM((chunks, per_dest, 2 * ne, bands, owned, LANES), f32),
            pltpu.VMEM((slots, bands, held, LANES), f32),
            pltpu.VMEM((slots, held, LANES), f32),
            pltpu.VMEM((slots, bands + 1, held, LANES), f32),
            pltpu.VMEM((ITERS, ne, held, LANES), f32),
            dma((loads,)),
            dma((5,)),
            pltpu.SemaphoreType.REGULAR((len(bits(ne)) + len(bits(nb)) - 1,)),
            dma((4,)),
            dma((count_of,)),
            dma((count_of,)),
            dma((chunks,)),
            dma((ITERS,)),
        ],
        compiler_params=pltpu.CompilerParams(
            collective_id=0, has_side_effects=True, vmem_limit_bytes=58 * 2**20
        ),
    )(visit_flux.transpose(0, 2, 1, 3), visit_precision.transpose(0, 2, 1, 3), visit_live,
      footprint, source_count, spectra_init.transpose(2, 0, 1), morphology_init)
    coadd, spectra, morphology = pl.pallas_call(
        hand_over,
        out_shape=(
            jax.ShapeDtypeStruct((bands, owned, pix_part), f32),
            jax.ShapeDtypeStruct((bands, owned, slots), f32),
            jax.ShapeDtypeStruct((owned, slots, pix_part), f32),
        ),
        in_specs=[vmem] * 3,
        out_specs=(hbm,) * 3,
        scratch_shapes=[dma((3,))],
        compiler_params=pltpu.CompilerParams(vmem_limit_bytes=8 * 2**20),
    )(*parts)
    return coadd.transpose(1, 0, 2), spectra.transpose(1, 2, 0), morphology


def on_device(
    visit_flux, visit_precision, visit_live, footprint, source_count, spectra_init, morphology_init
):
    weights = visit_precision.astype(jnp.float32) * visit_live.astype(jnp.float32)[:, :, None, None]
    numerator = jnp.sum(weights * visit_flux.astype(jnp.float32), axis=0)
    weight_sum = jnp.sum(weights, axis=0)
    pix_part = morphology_init.shape[2]
    owned = morphology_init.shape[0]
    numerator, weight_sum = (
        lax.psum_scatter(numerator, "epoch", scatter_dimension=2, tiled=True),
        lax.psum_scatter(weight_sum, "epoch", scatter_dimension=2, tiled=True),
    )
    every_blend, band_count, piece = numerator.shape
    numerator = numerator.reshape(every_blend, band_count, 1, piece)
    weight_sum = weight_sum.reshape(every_blend, band_count, 1, piece)
    numerator, weight_sum = (
        lax.all_to_all(numerator, "blend", split_axis=0, concat_axis=2, tiled=True),
        lax.all_to_all(weight_sum, "blend", split_axis=0, concat_axis=2, tiled=True),
    )
    blocks = numerator.shape[2]
    numerator = numerator.reshape(owned, band_count, blocks, 1, piece)
    weight_sum = weight_sum.reshape(owned, band_count, blocks, 1, piece)
    numerator, weight_sum = (
        lax.all_to_all(numerator, "epoch", split_axis=2, concat_axis=3, tiled=True),
        lax.all_to_all(weight_sum, "epoch", split_axis=2, concat_axis=3, tiled=True),
    )
    numerator = numerator.reshape(owned, band_count, pix_part)
    weight_sum = weight_sum.reshape(owned, band_count, pix_part)
    coadd_flux = numerator / (1.0 + weight_sum)
    coverage = weight_sum / (1.0 + weight_sum)
    slots = footprint.shape[1]
    source_live = (jnp.arange(slots, dtype=jnp.int32)[None, :] < source_count[:, None]).astype(
        jnp.float32
    )
    footprint_mask = footprint.astype(jnp.float32) * source_live[:, :, None]
    live_count = source_count.astype(jnp.float32)
    morphology = morphology_init * footprint_mask
    spectra = spectra_init
    highest = lax.Precision.HIGHEST
    for iteration in range(ITERS):
        blend_model = jnp.einsum("bkc,bkp->bcp", spectra, morphology, precision=highest)
        residual = coverage * (coadd_flux - blend_model)
        morph_grad = jnp.einsum("bkc,bcp->bkp", spectra, residual, precision=highest)
        morph_step = 1.0 / (1.0 + live_count[:, None] * jnp.sum(spectra * spectra, axis=2))
        morphology = (
            jnp.maximum(0.0, morphology + morph_grad * morph_step[:, :, None]) * footprint_mask
        )
        blend_model = jnp.einsum("bkc,bkp->bcp", spectra, morphology, precision=highest)
        residual = coverage * (coadd_flux - blend_model)
        spectra_grad = jnp.einsum("bkp,bcp->bkc", morphology, residual, precision=highest)
        morph_norm = jnp.sum(morphology * morphology, axis=2)
        spectra_grad, morph_norm = lax.psum((spectra_grad, morph_norm), "epoch")
        spectra = jnp.maximum(
            0.0, spectra + spectra_grad / (1.0 + live_count[:, None] * morph_norm)[:, :, None]
        )
    return (coadd_flux, spectra, morphology)


def solution(mesh):
    ne, nb = mesh.shape["epoch"], mesh.shape["blend"]

    def step(visit_flux, visit_precision, visit_live, footprint, source_count, spectra_init,
             morphology_init):
        block, bands = visit_flux.shape[3], visit_flux.shape[2]
        owned, pix_part = morphology_init.shape[0], morphology_init.shape[2]
        fits = (
            block % (ne * LANES) == 0
            and pix_part % block == 0
            and factors(ne) == (2, 2)
            and nb == 2 * ne
            and pix_part == 2 * block
            and visit_flux.shape[1] == owned * nb
            and AHEAD <= block // (ne * LANES) * bands
            and morphology_init.shape[1] * (bands + 1) <= LANES
        )
        run = functools.partial(fused, ne, nb) if fits else on_device
        return run(visit_flux, visit_precision, visit_live, footprint, source_count, spectra_init,
                   morphology_init)

    in_specs = (
        P("epoch", None, None, "blend"),
        P("epoch", None, None, "blend"),
        P("epoch", None),
        P("blend", None, "epoch"),
        P("blend"),
        P("blend", None, None),
        P("blend", None, "epoch"),
    )
    out_specs = (P("blend", None, "epoch"), P("blend", None, None), P("blend", None, "epoch"))
    return jax.shard_map(
        step, mesh=mesh, in_specs=in_specs, out_specs=out_specs, check_vma=False
    )
```

```python
import functools

import jax
import jax.numpy as jnp
from jax import lax
from jax.experimental import pallas as pl
from jax.experimental.pallas import tpu as pltpu
from jax.sharding import PartitionSpec as P

ITERS = 2


LANES = 128
MESH = pl.DeviceIdType.MESH
CUTS = 3
AHEAD = 4
LAG = 3
ROUTES = (
    (0, 0, 1, 6), (0, 2, 1, 2),
    (1, 0, 0, 3), (1, 1, 0, 5),
    (2, 0, 0, 4), (2, 2, 1, 2), (2, 3, 1, 2),
    (3, 1, 0, 4), (3, 2, 1, 4),
)


def factors(count):
    rows = max(d for d in range(1, count + 1) if count % d == 0 and d * d <= count)
    return rows, count // rows


def cut(chunks, bands):
    step = max(1, bands // CUTS)
    return [
        (q, lo, min(bands, lo + step)) for q in range(chunks) for lo in range(0, bands, step)
    ]


def plan():
    unit, runs = {}, []
    for t, p, first, n in ROUTES:
        runs.append((first, p >> first & 1, p >> 1 - first & 1, t, p, unit.get(t, 0), n))
        unit[t] = unit.get(t, 0) + n
    slot, placed = 0, []
    for first, one, two, t, p, u, n in sorted(runs):
        placed.append((first, one, two, t, p, u, n, slot))
        slot += n
    return placed, slot


def span(runs):
    runs = list(runs)
    return (min(r[7] for r in runs), sum(r[6] for r in runs)) if runs else (0, 0)


def slots_of(runs):
    return [r[7] + k for r in runs for k in range(r[6])]


def bits(count):
    return [1 << k for k in range(count.bit_length() - 1)]


def flip(at, bit):
    return at + bit - 2 * bit * (at // bit % 2)


def coadd_kernel(
    flux_hbm, prec_hbm, live_hbm, foot_hbm, count_hbm, spec_hbm, morph_hbm,
    coadd_ref, spec_out, morph_ref,
    in_v, live_ref, foot_v, count_ref, spec_ref, flux_c, cover,
    stage, land1, land2, final, pieces, spectra, step_ref, acc, sums,
    in_sem, side_sem, near_sem, send_sem, s1_recv, s2_recv, s3_recv, ps_recv,
    *, ne, nb,
):
    visits, bands, every_blend, block = flux_hbm.shape
    owned, slots, pix_part = morph_hbm.shape
    chunks = in_v.shape[1]
    width = block // chunks
    per_dest = pix_part // block
    held = per_dest * owned
    e = lax.axis_index("epoch")
    j = lax.axis_index("blend")
    y, x = e // 2, e % 2
    home_e = j // per_dest
    home_slot = j % per_dest
    f32 = jnp.float32
    work = cut(chunks, bands)
    runs, slot_count = plan()
    place = (x + home_e) % 2 + (y + home_e // 2) % 2 * 2
    slot_at = []
    for to in range(ne):
        b0, b1 = (home_e + to) % 2, (home_e // 2 + to // 2) % 2
        spots = []
        for u in range(2 * ne):
            t0, t1, t2, t3 = (
                next(r[7] + u - r[5] for r in runs if r[3] == t and r[5] <= u < r[5] + r[6])
                for t in range(ne)
            )
            spots.append(t0 + b0 * (t1 - t0) + b1 * (t2 - t0) + b0 * b1 * (t3 - t2 - t1 + t0))
        slot_at.append(spots)
    count_of = len(work)
    loads = [w for w in work if w[0] == 0] + [(q, 0, bands) for q in range(1, chunks)]

    small = [
        pltpu.make_async_copy(src, dst, side_sem.at[k])
        for k, (src, dst) in enumerate(
            ((live_hbm, live_ref), (count_hbm, count_ref), (spec_hbm, spec_ref)))
    ]
    small[0].start()

    def in_copy(n):
        q, lo, hi = loads[n]
        window, some = pl.ds(q * width, width), pl.ds(lo, hi - lo)
        return [
            pltpu.make_async_copy(
                src.at[:, some, :, window], in_v.at[k, q, :, some], in_sem.at[n])
            for k, src in enumerate((prec_hbm, flux_hbm))
        ]

    def in_wait(n):
        q, lo, hi = loads[n]
        here = in_v.at[:, q, :, pl.ds(lo, hi - lo)]
        pltpu.make_async_copy(here, here, in_sem.at[n]).wait()

    for n in range(len(loads)):
        for copy in in_copy(n):
            copy.start()

    near = [(flip(e, bit), j) for bit in bits(ne)] + [(e, flip(j, bit)) for bit in bits(nb)]
    barrier = pltpu.get_barrier_semaphore()
    for other in near:
        pl.semaphore_signal(barrier, inc=1, device_id=other, device_id_type=MESH)

    def spread(k):
        if k > 1:
            pl.semaphore_wait(near_sem.at[k - 2], 1)
        if k < len(near):
            pl.semaphore_signal(
                near_sem.at[k - 1], inc=1, device_id=near[k], device_id_type=MESH)

    for copy in small[1:]:
        copy.start()
    side = []
    for s in range(per_dest):
        for b in range(owned):
            row = s * owned + b
            window = pl.ds(s * block, block)
            side.append(pltpu.make_async_copy(
                foot_hbm.at[b, :, window], foot_v.at[:, row, :], side_sem.at[3]))
            side.append(pltpu.make_async_copy(
                morph_hbm.at[b, :, window], morph_ref.at[:, row, :], side_sem.at[4]))

    small[0].wait()
    square_r = lax.broadcasted_iota(jnp.int32, (every_blend, every_blend), 0)
    square_c = lax.broadcasted_iota(jnp.int32, (every_blend, every_blend), 1)
    lives = []
    for v in range(visits):
        row = jnp.broadcast_to(live_ref[v : v + 1, :].astype(f32), (every_blend, every_blend))
        column = jnp.sum(jnp.where(square_r == square_c, row, 0.0), axis=1, keepdims=True)
        lives.append(jnp.broadcast_to(column, (every_blend, LANES)))

    def local_sum(i):
        q, lo, hi = work[i]
        for n, (r, start, _) in enumerate(loads):
            if r == q and start == lo:
                in_wait(n)

        def one(c, carry):
            for g in range(ne):
                lanes = slice(g * LANES, (g + 1) * LANES)
                num = None
                for v in range(visits):
                    w = in_v[0, q, v, c, :, lanes].astype(f32) * lives[v]
                    n = w * in_v[1, q, v, c, :, lanes].astype(f32)
                    num, wsum = (n, w) if num is None else (num + n, wsum + w)
                for k, total in enumerate((num, wsum)):
                    for to in range(ne):
                        stage[q, slot_at[to][k * ne + g], c] = total[to * held : (to + 1) * held, :]
            return carry

        lax.fori_loop(lo, hi, one, 0)

    def at_place(act):
        for p in range(ne):
            @pl.when(place == p)
            def _(p=p):
                act(p)

    def kept(p, first):
        return [r for r in runs if r[0] == first and r[1] == p >> first & 1]

    def given(p, first):
        return [r for r in runs if r[0] == first and r[1] != p >> first & 1]

    def passed(p, first):
        return [r for r in kept(p, first) if r[2] != p >> 1 - first & 1]

    def owned_at(p):
        return [r for r in runs if r[4] == p]

    def exchange(src, dst, i, sent, to, send, recv):
        q, lo, hi = work[i]
        first, n = span(sent)
        if n:
            piece = (q, pl.ds(first, n), pl.ds(lo, hi - lo))
            pltpu.make_async_remote_copy(
                src_ref=src.at[piece], dst_ref=dst.at[piece],
                send_sem=send_sem.at[send], recv_sem=recv.at[i],
                device_id=to, device_id_type=MESH,
            ).start()

    def arrive(ref, i, n, recv):
        q, lo, hi = work[i]
        if n:
            here = ref.at[q, pl.ds(0, n), pl.ds(lo, hi - lo)]
            pltpu.make_async_copy(here, here, recv.at[i]).wait()

    def s1_start(i):
        def act(p):
            for first in range(2):
                exchange(stage, land1, i, given(p, first), near[first], 0, s1_recv)

        at_place(act)

    def s2_start(i):
        q, lo, hi = work[i]

        def act(p):
            mine = slots_of(kept(p, 0) + kept(p, 1))
            arrive(land1, i, len(mine), s1_recv)

            def add(c, carry):
                for k in mine:
                    stage[q, k, c] = stage[q, k, c] + land1[q, k, c]
                return carry

            lax.fori_loop(lo, hi, add, 0)
            for first in range(2):
                exchange(stage, land2, i, passed(p, first), near[1 - first], 1, s2_recv)

        at_place(act)

    def s3_start(i):
        q, lo, hi = work[i]
        some = pl.ds(lo, hi - lo)

        def act(p):
            mine = slots_of(owned_at(p))
            arrive(land2, i, len(mine), s2_recv)

            def add(c, carry):
                for k in mine:
                    v = stage[q, k, c] + land2[q, k, c]
                    for to in range(per_dest):
                        final[q, to, k, c] = v[to * owned : (to + 1) * owned, :]
                return carry

            lax.fori_loop(lo, hi, add, 0)
            for order in range(per_dest):
                for _, _, _, t, _, u, n, first in sorted(owned_at(p), key=lambda r: -r[3]):
                    over = j
                    for bit in bits(ne):
                        if t & bit:
                            over = flip(over, bit * per_dest)
                    stays = p == 0 and t == 0
                    to = flip(over, 1) if stays else over - home_slot + order
                    core = to % per_dest if stays else order
                    src = final.at[q, core, pl.ds(first, n), some]
                    dst = pieces.at[q, home_slot, pl.ds(u, n), some]
                    if stays and order:
                        src = final.at[q, home_slot, pl.ds(first, n), some]
                        pltpu.make_async_copy(src, dst, s3_recv.at[q]).start()
                    else:
                        pltpu.make_async_remote_copy(
                            src_ref=src, dst_ref=dst,
                            send_sem=send_sem.at[2], recv_sem=s3_recv.at[q],
                            device_id=(home_e, to), device_id_type=MESH,
                        ).start()

        at_place(act)

    sub = lax.broadcasted_iota(jnp.int32, (held, LANES), 0)
    lane = lax.broadcasted_iota(jnp.int32, (held, LANES), 1)
    state = []

    def steps():
        for k in range(slots):
            norm = None
            for c in range(bands):
                s = spectra[k, c]
                norm = s * s if norm is None else norm + s * s
            step_ref[k] = 1.0 / (1.0 + state[1] * norm)

    group = 2

    def deblend(start, first):
        runs = [
            pl.ds(pl.multiple_of(start + t * LANES, LANES), LANES) for t in range(group)
        ]

        def masks(k):
            live = jnp.where(state[0] > k, 1.0, 0.0).astype(f32)
            return [foot_v[k, :, px].astype(f32) * live for px in runs]

        def residual(morph):
            res = []
            for c in range(bands):
                model = [None] * group
                for k in range(slots):
                    s = spectra[k, c]
                    for t in range(group):
                        v = s * morph[k][t]
                        model[t] = v if k == 0 else model[t] + v
                res.append([
                    cover[c, :, px] * (flux_c[c, :, px] - model[t]) for t, px in enumerate(runs)
                ])
            return res

        morph = []
        for k in range(slots):
            m = [morph_ref[k, :, px] for px in runs]
            morph.append([a * b for a, b in zip(m, masks(k))] if first else m)
        res = residual(morph)
        for k in range(slots):
            mask = masks(k)
            grad = [None] * group
            for c in range(bands):
                s = spectra[k, c]
                for t in range(group):
                    v = s * res[c][t]
                    grad[t] = v if c == 0 else grad[t] + v
            step = step_ref[k]
            for t, px in enumerate(runs):
                m = jnp.maximum(0.0, morph[k][t] + grad[t] * step) * mask[t]
                morph[k][t] = m
                morph_ref[k, :, px] = m
        res = residual(morph)
        for k in range(slots):
            for c in range(bands):
                v = acc[k, c]
                for t in range(group):
                    v = v + morph[k][t] * res[c][t]
                acc[k, c] = v
            v = acc[k, bands]
            for t in range(group):
                v = v + morph[k][t] * morph[k][t]
            acc[k, bands] = v

    def finish(q):
        pltpu.make_async_copy(pieces.at[q], pieces.at[q], s3_recv.at[q]).wait()

        def unpack(c, carry):
            for s in range(per_dest):
                rows = slice(s * owned, (s + 1) * owned)
                for g in range(ne):
                    wsum = pieces[q, s, ne + g, c]
                    inv = 1.0 / (1.0 + wsum)
                    flux = pieces[q, s, g, c] * inv
                    px = q * width + g * LANES
                    coadd_ref[c, :, s * block + px : s * block + px + LANES] = flux
                    flux_c[c, rows, px : px + LANES] = flux
                    cover[c, rows, px : px + LANES] = wsum * inv
            return carry

        lax.fori_loop(0, bands, unpack, 0)

        def go(i, carry):
            deblend(q * width + i * (group * LANES), True)
            return carry

        lax.fori_loop(0, width // (group * LANES), go, 0)

    def ps_copy(it, d):
        to = lax.rem(e + d, ne)
        return pltpu.make_async_remote_copy(
            src_ref=sums.at[it, 0], dst_ref=sums.at[it, d],
            send_sem=send_sem.at[3], recv_sem=ps_recv.at[it],
            device_id=(to, j), device_id_type=MESH,
        )

    def drain():
        def act(p):
            for k, n in enumerate((
                span(given(p, 0))[1] + span(given(p, 1))[1],
                span(passed(p, 0))[1] + span(passed(p, 1))[1],
            )):
                if n:
                    sent = stage.at[:, pl.ds(0, n)]
                    pltpu.make_async_copy(sent, sent, send_sem.at[k]).wait()
            n = sum(r[6] * (per_dest - (p == 0 and r[3] == 0)) for r in owned_at(p))
            sent = final.at[:, 0, pl.ds(0, n)]
            pltpu.make_async_copy(sent, sent, send_sem.at[2]).wait()

        at_place(act)

    def update(it):
        packed = jnp.zeros((held, LANES), f32)
        for k in range(slots):
            for c in range(bands + 1):
                whole = jnp.sum(acc[k, c], axis=1, keepdims=True)
                packed = jnp.where(lane == k * (bands + 1) + c, whole, packed)
        sums[it, 0] = packed
        for d in range(1, ne):
            ps_copy(it, d).start()
        if it == ITERS - 1:
            drain()
        arrived = sums.at[it, pl.ds(1, ne - 1)]
        pltpu.make_async_copy(arrived, arrived, ps_recv.at[it]).wait()
        whole = None
        for o in range(ne):
            v = sums[it, lax.rem(e - o + ne, ne)]
            whole = v if whole is None else whole + v
        one = whole[0:owned, :]
        for s in range(1, per_dest):
            one = one + whole[s * owned : (s + 1) * owned, :]
        whole = jnp.concatenate([one] * per_dest, axis=0)
        for k in range(slots):
            at = k * (bands + 1)
            norm = jnp.broadcast_to(whole[:, at + bands : at + bands + 1], (held, LANES))
            scale = 1.0 / (1.0 + state[1] * norm)
            for c in range(bands):
                grad = jnp.broadcast_to(whole[:, at + c : at + c + 1], (held, LANES))
                spectra[k, c] = jnp.maximum(0.0, spectra[k, c] + grad * scale)

    local_sum(0)
    pl.semaphore_wait(barrier, len(near))
    s1_start(0)
    spread(1)
    for i in range(1, min(AHEAD, count_of)):
        local_sum(i)
        s1_start(i)
        if i + 1 < len(near):
            spread(i + 1)
    for copy in side:
        copy.start()

    for copy in small[1:]:
        copy.wait()
    count = jnp.zeros((held, LANES), jnp.int32)
    for b in range(owned):
        count = jnp.where(lax.rem(sub, owned) == b, count_ref[b], count)
    state.extend((count, count.astype(f32)))
    acc[...] = jnp.zeros_like(acc)
    for k in range(slots):
        for c in range(bands):
            start = jnp.broadcast_to(spec_ref[c, :, k : k + 1], (owned, LANES))
            spectra[k, c] = jnp.concatenate([start] * per_dest, axis=0)
    steps()

    for k in range(min(AHEAD, count_of) + 1, len(near)):
        spread(k)
    for i in range(count_of + LAG):
        if i < count_of:
            s2_start(i)
        if i + AHEAD < count_of:
            local_sum(i + AHEAD)
            s1_start(i + AHEAD)
        if i == LAG:
            spread(len(near))
        if 0 <= i - LAG < count_of:
            s3_start(i - LAG)
    for done, copies in ((foot_v, 3), (morph_ref, 4)):
        pltpu.make_async_copy(done, done, side_sem.at[copies]).wait()
    for q in range(chunks):
        finish(q)

    update(0)
    for it in range(1, ITERS):
        steps()
        acc[...] = jnp.zeros_like(acc)

        def again(i, carry):
            deblend(i * (group * LANES), False)
            return carry

        lax.fori_loop(0, block // (group * LANES), again, 0)
        update(it)
    for c in range(bands):
        out = spectra[0, c]
        for k in range(1, slots):
            out = jnp.where(lane == k, spectra[k, c], out)
        spec_out[c] = out[0:owned, :slots]

    gone = sums.at[:, pl.ds(1, ne - 1)]
    pltpu.make_async_copy(gone, gone, send_sem.at[3]).wait()


def hand_over(coadd_in, spec_in, morph_in, coadd_out, spec_out, morph_out, sems):
    owned, _, pix_part = morph_out.shape
    _, held, block = morph_in.shape
    for row in range(held):
        pltpu.make_async_copy(
            morph_in.at[:, row, :],
            morph_out.at[row % owned, :, pl.ds(row // owned * block, block)], sems.at[2]).start()
    others = [pltpu.make_async_copy(coadd_in, coadd_out, sems.at[0]),
              pltpu.make_async_copy(spec_in, spec_out, sems.at[1])]
    for copy in others:
        copy.start()
    pltpu.make_async_copy(morph_in, morph_in, sems.at[2]).wait()
    for copy in others:
        copy.wait()


def fused(ne, nb, visit_flux, visit_precision, visit_live, footprint, source_count, spectra_init,
          morphology_init):
    visits, every_blend, bands, block = visit_flux.shape
    owned, slots, pix_part = morphology_init.shape
    width = ne * LANES
    chunks = block // width
    per_dest = pix_part // block
    held = per_dest * owned
    count_of = len(cut(chunks, bands))
    loads = count_of // chunks + chunks - 1
    slot_count = plan()[1]
    f32 = jnp.float32
    vmem, hbm = (pl.BlockSpec(memory_space=s) for s in (pltpu.VMEM, pl.ANY))
    dma = pltpu.SemaphoreType.DMA
    parts = pl.pallas_call(
        functools.partial(coadd_kernel, ne=ne, nb=nb),
        out_shape=(
            pltpu.VMEM((bands, owned, pix_part), f32),
            pltpu.VMEM((bands, owned, slots), f32),
            pltpu.VMEM((slots, held, block), f32),
        ),
        in_specs=[hbm] * 7,
        out_specs=(vmem, vmem, vmem),
        scratch_shapes=[
            pltpu.VMEM((2, chunks, visits, bands, every_blend, width), visit_flux.dtype),
            pltpu.VMEM(visit_live.shape, jnp.int32),
            pltpu.VMEM((slots, held, block), jnp.int32),
            pltpu.SMEM(source_count.shape, jnp.int32),
            pltpu.VMEM((bands, owned, slots), f32),
            pltpu.VMEM((bands, held, block), f32),
            pltpu.VMEM((bands, held, block), f32),
            pltpu.VMEM((chunks, slot_count, bands, held, LANES), f32),
            pltpu.VMEM((chunks, slot_count, bands, held, LANES), f32),
            pltpu.VMEM((chunks, slot_count, bands, held, LANES), f32),
            pltpu.VMEM((chunks, per_dest, slot_count, bands, owned, LANES), f32),
            pltpu.VMEM((chunks, per_dest, 2 * ne, bands, owned, LANES), f32),
            pltpu.VMEM((slots, bands, held, LANES), f32),
            pltpu.VMEM((slots, held, LANES), f32),
            pltpu.VMEM((slots, bands + 1, held, LANES), f32),
            pltpu.VMEM((ITERS, ne, held, LANES), f32),
            dma((loads,)),
            dma((5,)),
            pltpu.SemaphoreType.REGULAR((len(bits(ne)) + len(bits(nb)) - 1,)),
            dma((4,)),
            dma((count_of,)),
            dma((count_of,)),
            dma((chunks,)),
            dma((ITERS,)),
        ],
        compiler_params=pltpu.CompilerParams(
            collective_id=0, has_side_effects=True, vmem_limit_bytes=58 * 2**20
        ),
    )(visit_flux.transpose(0, 2, 1, 3), visit_precision.transpose(0, 2, 1, 3), visit_live,
      footprint, source_count, spectra_init.transpose(2, 0, 1), morphology_init)
    coadd, spectra, morphology = pl.pallas_call(
        hand_over,
        out_shape=(
            jax.ShapeDtypeStruct((bands, owned, pix_part), f32),
            jax.ShapeDtypeStruct((bands, owned, slots), f32),
            jax.ShapeDtypeStruct((owned, slots, pix_part), f32),
        ),
        in_specs=[vmem] * 3,
        out_specs=(hbm,) * 3,
        scratch_shapes=[dma((3,))],
        compiler_params=pltpu.CompilerParams(vmem_limit_bytes=8 * 2**20),
    )(*parts)
    return coadd.transpose(1, 0, 2), spectra.transpose(1, 2, 0), morphology


def on_device(
    visit_flux, visit_precision, visit_live, footprint, source_count, spectra_init, morphology_init
):
    weights = visit_precision.astype(jnp.float32) * visit_live.astype(jnp.float32)[:, :, None, None]
    numerator = jnp.sum(weights * visit_flux.astype(jnp.float32), axis=0)
    weight_sum = jnp.sum(weights, axis=0)
    pix_part = morphology_init.shape[2]
    owned = morphology_init.shape[0]
    numerator, weight_sum = (
        lax.psum_scatter(numerator, "epoch", scatter_dimension=2, tiled=True),
        lax.psum_scatter(weight_sum, "epoch", scatter_dimension=2, tiled=True),
    )
    every_blend, band_count, piece = numerator.shape
    numerator = numerator.reshape(every_blend, band_count, 1, piece)
    weight_sum = weight_sum.reshape(every_blend, band_count, 1, piece)
    numerator, weight_sum = (
        lax.all_to_all(numerator, "blend", split_axis=0, concat_axis=2, tiled=True),
        lax.all_to_all(weight_sum, "blend", split_axis=0, concat_axis=2, tiled=True),
    )
    blocks = numerator.shape[2]
    numerator = numerator.reshape(owned, band_count, blocks, 1, piece)
    weight_sum = weight_sum.reshape(owned, band_count, blocks, 1, piece)
    numerator, weight_sum = (
        lax.all_to_all(numerator, "epoch", split_axis=2, concat_axis=3, tiled=True),
        lax.all_to_all(weight_sum, "epoch", split_axis=2, concat_axis=3, tiled=True),
    )
    numerator = numerator.reshape(owned, band_count, pix_part)
    weight_sum = weight_sum.reshape(owned, band_count, pix_part)
    coadd_flux = numerator / (1.0 + weight_sum)
    coverage = weight_sum / (1.0 + weight_sum)
    slots = footprint.shape[1]
    source_live = (jnp.arange(slots, dtype=jnp.int32)[None, :] < source_count[:, None]).astype(
        jnp.float32
    )
    footprint_mask = footprint.astype(jnp.float32) * source_live[:, :, None]
    live_count = source_count.astype(jnp.float32)
    morphology = morphology_init * footprint_mask
    spectra = spectra_init
    highest = lax.Precision.HIGHEST
    for iteration in range(ITERS):
        blend_model = jnp.einsum("bkc,bkp->bcp", spectra, morphology, precision=highest)
        residual = coverage * (coadd_flux - blend_model)
        morph_grad = jnp.einsum("bkc,bcp->bkp", spectra, residual, precision=highest)
        morph_step = 1.0 / (1.0 + live_count[:, None] * jnp.sum(spectra * spectra, axis=2))
        morphology = (
            jnp.maximum(0.0, morphology + morph_grad * morph_step[:, :, None]) * footprint_mask
        )
        blend_model = jnp.einsum("bkc,bkp->bcp", spectra, morphology, precision=highest)
        residual = coverage * (coadd_flux - blend_model)
        spectra_grad = jnp.einsum("bkp,bcp->bkc", morphology, residual, precision=highest)
        morph_norm = jnp.sum(morphology * morphology, axis=2)
        spectra_grad, morph_norm = lax.psum((spectra_grad, morph_norm), "epoch")
        spectra = jnp.maximum(
            0.0, spectra + spectra_grad / (1.0 + live_count[:, None] * morph_norm)[:, :, None]
        )
    return (coadd_flux, spectra, morphology)


def solution(mesh):
    ne, nb = mesh.shape["epoch"], mesh.shape["blend"]

    def step(visit_flux, visit_precision, visit_live, footprint, source_count, spectra_init,
             morphology_init):
        block, bands = visit_flux.shape[3], visit_flux.shape[2]
        owned, pix_part = morphology_init.shape[0], morphology_init.shape[2]
        fits = (
            block % (ne * LANES) == 0
            and pix_part % block == 0
            and factors(ne) == (2, 2)
            and nb == 2 * ne
            and pix_part == 2 * block
            and visit_flux.shape[1] == owned * nb
            and AHEAD <= block // (ne * LANES) * bands
            and morphology_init.shape[1] * (bands + 1) <= LANES
        )
        run = functools.partial(fused, ne, nb) if fits else on_device
        return run(visit_flux, visit_precision, visit_live, footprint, source_count, spectra_init,
                   morphology_init)

    in_specs = (
        P("epoch", None, None, "blend"),
        P("epoch", None, None, "blend"),
        P("epoch", None),
        P("blend", None, "epoch"),
        P("blend"),
        P("blend", None, None),
        P("blend", None, "epoch"),
    )
    out_specs = (P("blend", None, "epoch"), P("blend", None, None), P("blend", None, "epoch"))
    return jax.shard_map(
        step, mesh=mesh, in_specs=in_specs, out_specs=out_specs, check_vma=False
    )
```

```python
import functools

import jax
import jax.numpy as jnp
from jax import lax
from jax.experimental import pallas as pl
from jax.experimental.pallas import tpu as pltpu
from jax.sharding import PartitionSpec as P

ITERS = 2


LANES = 128
MESH = pl.DeviceIdType.MESH
CUTS = 3
AHEAD = 4
LAG = 3
ROUTES = ((0, 0, 0, 6), (0, 1, 0, 1), (0, 2, 1, 1), (1, 0, 1, 8), (2, 1, 0, 1), (2, 2, 1, 7), (3, 1, 0, 5), (3, 3, 0, 3))


def factors(count):
    rows = max(d for d in range(1, count + 1) if count % d == 0 and d * d <= count)
    return rows, count // rows


def cut(chunks, bands):
    step = max(1, bands // CUTS)
    return [
        (q, lo, min(bands, lo + step)) for q in range(chunks) for lo in range(0, bands, step)
    ]


def plan():
    unit, runs = {}, []
    for t, p, first, n in ROUTES:
        runs.append((first, p >> first & 1, p >> 1 - first & 1, t, p, unit.get(t, 0), n))
        unit[t] = unit.get(t, 0) + n
    slot, placed = 0, []
    for first, one, two, t, p, u, n in sorted(runs):
        placed.append((first, one, two, t, p, u, n, slot))
        slot += n
    return placed, slot


def span(runs):
    runs = list(runs)
    return (min(r[7] for r in runs), sum(r[6] for r in runs)) if runs else (0, 0)


def slots_of(runs):
    return [r[7] + k for r in runs for k in range(r[6])]


def bits(count):
    return [1 << k for k in range(count.bit_length() - 1)]


def flip(at, bit):
    return at + bit - 2 * bit * (at // bit % 2)


def coadd_kernel(
    flux_hbm, prec_hbm, live_hbm, foot_hbm, count_hbm, spec_hbm, morph_hbm,
    coadd_ref, spec_out, morph_ref,
    in_v, live_ref, foot_v, count_ref, spec_ref, flux_c, cover,
    stage, land1, land2, final, pieces, spectra, step_ref, acc, sums,
    in_sem, side_sem, near_sem, send_sem, s1_recv, s2_recv, s3_recv, ps_recv,
    *, ne, nb,
):
    visits, bands, every_blend, block = flux_hbm.shape
    owned, slots, pix_part = morph_hbm.shape
    chunks = in_v.shape[1]
    width = block // chunks
    per_dest = pix_part // block
    held = per_dest * owned
    e = lax.axis_index("epoch")
    j = lax.axis_index("blend")
    y, x = e // 2, e % 2
    home_e = j // per_dest
    home_slot = j % per_dest
    f32 = jnp.float32
    work = cut(chunks, bands)
    runs, slot_count = plan()
    place = (x + home_e) % 2 + (y + home_e // 2) % 2 * 2
    slot_at = []
    for to in range(ne):
        b0, b1 = (home_e + to) % 2, (home_e // 2 + to // 2) % 2
        spots = []
        for u in range(2 * ne):
            t0, t1, t2, t3 = (
                next(r[7] + u - r[5] for r in runs if r[3] == t and r[5] <= u < r[5] + r[6])
                for t in range(ne)
            )
            spots.append(t0 + b0 * (t1 - t0) + b1 * (t2 - t0) + b0 * b1 * (t3 - t2 - t1 + t0))
        slot_at.append(spots)
    count_of = len(work)
    loads = [w for w in work if w[0] == 0] + [(q, 0, bands) for q in range(1, chunks)]

    small = [
        pltpu.make_async_copy(src, dst, side_sem.at[k])
        for k, (src, dst) in enumerate(
            ((live_hbm, live_ref), (count_hbm, count_ref), (spec_hbm, spec_ref)))
    ]
    small[0].start()

    def in_copy(n):
        q, lo, hi = loads[n]
        window, some = pl.ds(q * width, width), pl.ds(lo, hi - lo)
        return [
            pltpu.make_async_copy(
                src.at[:, some, :, window], in_v.at[k, q, :, some], in_sem.at[n])
            for k, src in enumerate((prec_hbm, flux_hbm))
        ]

    def in_wait(n):
        q, lo, hi = loads[n]
        here = in_v.at[:, q, :, pl.ds(lo, hi - lo)]
        pltpu.make_async_copy(here, here, in_sem.at[n]).wait()

    for n in range(len(loads)):
        for copy in in_copy(n):
            copy.start()

    near = [(flip(e, bit), j) for bit in bits(ne)] + [(e, flip(j, bit)) for bit in bits(nb)]
    barrier = pltpu.get_barrier_semaphore()
    for other in near:
        pl.semaphore_signal(barrier, inc=1, device_id=other, device_id_type=MESH)

    def spread(k):
        if k > 1:
            pl.semaphore_wait(near_sem.at[k - 2], 1)
        if k < len(near):
            pl.semaphore_signal(
                near_sem.at[k - 1], inc=1, device_id=near[k], device_id_type=MESH)

    for copy in small[1:]:
        copy.start()
    side = []
    for s in range(per_dest):
        for b in range(owned):
            row = s * owned + b
            window = pl.ds(s * block, block)
            side.append(pltpu.make_async_copy(
                foot_hbm.at[b, :, window], foot_v.at[:, row, :], side_sem.at[3]))
            side.append(pltpu.make_async_copy(
                morph_hbm.at[b, :, window], morph_ref.at[:, row, :], side_sem.at[4]))

    small[0].wait()
    square_r = lax.broadcasted_iota(jnp.int32, (every_blend, every_blend), 0)
    square_c = lax.broadcasted_iota(jnp.int32, (every_blend, every_blend), 1)
    lives = []
    for v in range(visits):
        row = jnp.broadcast_to(live_ref[v : v + 1, :].astype(f32), (every_blend, every_blend))
        column = jnp.sum(jnp.where(square_r == square_c, row, 0.0), axis=1, keepdims=True)
        lives.append(jnp.broadcast_to(column, (every_blend, LANES)))

    def local_sum(i):
        q, lo, hi = work[i]
        for n, (r, start, _) in enumerate(loads):
            if r == q and start == lo:
                in_wait(n)

        def one(c, carry):
            for g in range(ne):
                lanes = slice(g * LANES, (g + 1) * LANES)
                num = None
                for v in range(visits):
                    w = in_v[0, q, v, c, :, lanes].astype(f32) * lives[v]
                    n = w * in_v[1, q, v, c, :, lanes].astype(f32)
                    num, wsum = (n, w) if num is None else (num + n, wsum + w)
                for k, total in enumerate((num, wsum)):
                    for to in range(ne):
                        stage[q, slot_at[to][k * ne + g], c] = total[to * held : (to + 1) * held, :]
            return carry

        lax.fori_loop(lo, hi, one, 0)

    def at_place(act):
        for p in range(ne):
            @pl.when(place == p)
            def _(p=p):
                act(p)

    def kept(p, first):
        return [r for r in runs if r[0] == first and r[1] == p >> first & 1]

    def given(p, first):
        return [r for r in runs if r[0] == first and r[1] != p >> first & 1]

    def passed(p, first):
        return [r for r in kept(p, first) if r[2] != p >> 1 - first & 1]

    def owned_at(p):
        return [r for r in runs if r[4] == p]

    def exchange(src, dst, i, sent, to, send, recv):
        q, lo, hi = work[i]
        first, n = span(sent)
        if n:
            piece = (q, pl.ds(first, n), pl.ds(lo, hi - lo))
            pltpu.make_async_remote_copy(
                src_ref=src.at[piece], dst_ref=dst.at[piece],
                send_sem=send_sem.at[send], recv_sem=recv.at[i],
                device_id=to, device_id_type=MESH,
            ).start()

    def arrive(ref, i, n, recv):
        q, lo, hi = work[i]
        if n:
            here = ref.at[q, pl.ds(0, n), pl.ds(lo, hi - lo)]
            pltpu.make_async_copy(here, here, recv.at[i]).wait()

    def s1_start(i):
        def act(p):
            for first in range(2):
                exchange(stage, land1, i, given(p, first), near[first], 0, s1_recv)

        at_place(act)

    def s2_start(i):
        q, lo, hi = work[i]

        def act(p):
            mine = slots_of(kept(p, 0) + kept(p, 1))
            arrive(land1, i, len(mine), s1_recv)

            def add(c, carry):
                for k in mine:
                    stage[q, k, c] = stage[q, k, c] + land1[q, k, c]
                return carry

            lax.fori_loop(lo, hi, add, 0)
            for first in range(2):
                exchange(stage, land2, i, passed(p, first), near[1 - first], 1, s2_recv)

        at_place(act)

    def s3_start(i):
        q, lo, hi = work[i]
        some = pl.ds(lo, hi - lo)

        def act(p):
            mine = slots_of(owned_at(p))
            arrive(land2, i, len(mine), s2_recv)

            def add(c, carry):
                for k in mine:
                    v = stage[q, k, c] + land2[q, k, c]
                    for to in range(per_dest):
                        final[q, to, k, c] = v[to * owned : (to + 1) * owned, :]
                return carry

            lax.fori_loop(lo, hi, add, 0)
            for order in range(per_dest):
                for _, _, _, t, _, u, n, first in sorted(owned_at(p), key=lambda r: -r[3]):
                    over = j
                    for bit in bits(ne):
                        if t & bit:
                            over = flip(over, bit * per_dest)
                    stays = p == 0 and t == 0
                    to = flip(over, 1) if stays else over - home_slot + order
                    core = to % per_dest if stays else order
                    src = final.at[q, core, pl.ds(first, n), some]
                    dst = pieces.at[q, home_slot, pl.ds(u, n), some]
                    if stays and order:
                        src = final.at[q, home_slot, pl.ds(first, n), some]
                        pltpu.make_async_copy(src, dst, s3_recv.at[q]).start()
                    else:
                        pltpu.make_async_remote_copy(
                            src_ref=src, dst_ref=dst,
                            send_sem=send_sem.at[2], recv_sem=s3_recv.at[q],
                            device_id=(home_e, to), device_id_type=MESH,
                        ).start()

        at_place(act)

    sub = lax.broadcasted_iota(jnp.int32, (held, LANES), 0)
    lane = lax.broadcasted_iota(jnp.int32, (held, LANES), 1)
    state = []

    def steps():
        for k in range(slots):
            norm = None
            for c in range(bands):
                s = spectra[k, c]
                norm = s * s if norm is None else norm + s * s
            step_ref[k] = 1.0 / (1.0 + state[1] * norm)

    group = 2

    def deblend(start, first):
        runs = [
            pl.ds(pl.multiple_of(start + t * LANES, LANES), LANES) for t in range(group)
        ]

        def masks(k):
            live = jnp.where(state[0] > k, 1.0, 0.0).astype(f32)
            return [foot_v[k, :, px].astype(f32) * live for px in runs]

        def residual(morph):
            res = []
            for c in range(bands):
                model = [None] * group
                for k in range(slots):
                    s = spectra[k, c]
                    for t in range(group):
                        v = s * morph[k][t]
                        model[t] = v if k == 0 else model[t] + v
                res.append([
                    cover[c, :, px] * (flux_c[c, :, px] - model[t]) for t, px in enumerate(runs)
                ])
            return res

        morph = []
        for k in range(slots):
            m = [morph_ref[k, :, px] for px in runs]
            morph.append([a * b for a, b in zip(m, masks(k))] if first else m)
        res = residual(morph)
        for k in range(slots):
            mask = masks(k)
            grad = [None] * group
            for c in range(bands):
                s = spectra[k, c]
                for t in range(group):
                    v = s * res[c][t]
                    grad[t] = v if c == 0 else grad[t] + v
            step = step_ref[k]
            for t, px in enumerate(runs):
                m = jnp.maximum(0.0, morph[k][t] + grad[t] * step) * mask[t]
                morph[k][t] = m
                morph_ref[k, :, px] = m
        res = residual(morph)
        for k in range(slots):
            for c in range(bands):
                v = acc[k, c]
                for t in range(group):
                    v = v + morph[k][t] * res[c][t]
                acc[k, c] = v
            v = acc[k, bands]
            for t in range(group):
                v = v + morph[k][t] * morph[k][t]
            acc[k, bands] = v

    def finish(q):
        pltpu.make_async_copy(pieces.at[q], pieces.at[q], s3_recv.at[q]).wait()

        def unpack(c, carry):
            for s in range(per_dest):
                rows = slice(s * owned, (s + 1) * owned)
                for g in range(ne):
                    wsum = pieces[q, s, ne + g, c]
                    inv = 1.0 / (1.0 + wsum)
                    flux = pieces[q, s, g, c] * inv
                    px = q * width + g * LANES
                    coadd_ref[c, :, s * block + px : s * block + px + LANES] = flux
                    flux_c[c, rows, px : px + LANES] = flux
                    cover[c, rows, px : px + LANES] = wsum * inv
            return carry

        lax.fori_loop(0, bands, unpack, 0)

        def go(i, carry):
            deblend(q * width + i * (group * LANES), True)
            return carry

        lax.fori_loop(0, width // (group * LANES), go, 0)

    def ps_copy(it, d):
        to = lax.rem(e + d, ne)
        return pltpu.make_async_remote_copy(
            src_ref=sums.at[it, 0], dst_ref=sums.at[it, d],
            send_sem=send_sem.at[3], recv_sem=ps_recv.at[it],
            device_id=(to, j), device_id_type=MESH,
        )

    def drain():
        def act(p):
            for k, n in enumerate((
                span(given(p, 0))[1] + span(given(p, 1))[1],
                span(passed(p, 0))[1] + span(passed(p, 1))[1],
            )):
                if n:
                    sent = stage.at[:, pl.ds(0, n)]
                    pltpu.make_async_copy(sent, sent, send_sem.at[k]).wait()
            n = sum(r[6] * (per_dest - (p == 0 and r[3] == 0)) for r in owned_at(p))
            sent = final.at[:, 0, pl.ds(0, n)]
            pltpu.make_async_copy(sent, sent, send_sem.at[2]).wait()

        at_place(act)

    def update(it):
        packed = jnp.zeros((held, LANES), f32)
        for k in range(slots):
            for c in range(bands + 1):
                whole = jnp.sum(acc[k, c], axis=1, keepdims=True)
                packed = jnp.where(lane == k * (bands + 1) + c, whole, packed)
        sums[it, 0] = packed
        for d in range(1, ne):
            ps_copy(it, d).start()
        if it == ITERS - 1:
            drain()
        arrived = sums.at[it, pl.ds(1, ne - 1)]
        pltpu.make_async_copy(arrived, arrived, ps_recv.at[it]).wait()
        whole = None
        for o in range(ne):
            v = sums[it, lax.rem(e - o + ne, ne)]
            whole = v if whole is None else whole + v
        one = whole[0:owned, :]
        for s in range(1, per_dest):
            one = one + whole[s * owned : (s + 1) * owned, :]
        whole = jnp.concatenate([one] * per_dest, axis=0)
        for k in range(slots):
            at = k * (bands + 1)
            norm = jnp.broadcast_to(whole[:, at + bands : at + bands + 1], (held, LANES))
            scale = 1.0 / (1.0 + state[1] * norm)
            for c in range(bands):
                grad = jnp.broadcast_to(whole[:, at + c : at + c + 1], (held, LANES))
                spectra[k, c] = jnp.maximum(0.0, spectra[k, c] + grad * scale)

    local_sum(0)
    pl.semaphore_wait(barrier, len(near))
    s1_start(0)
    spread(1)
    for i in range(1, min(AHEAD, count_of)):
        local_sum(i)
        s1_start(i)
        if i + 1 < len(near):
            spread(i + 1)
    for copy in side:
        copy.start()

    for copy in small[1:]:
        copy.wait()
    count = jnp.zeros((held, LANES), jnp.int32)
    for b in range(owned):
        count = jnp.where(lax.rem(sub, owned) == b, count_ref[b], count)
    state.extend((count, count.astype(f32)))
    acc[...] = jnp.zeros_like(acc)
    for k in range(slots):
        for c in range(bands):
            start = jnp.broadcast_to(spec_ref[c, :, k : k + 1], (owned, LANES))
            spectra[k, c] = jnp.concatenate([start] * per_dest, axis=0)
    steps()

    for k in range(min(AHEAD, count_of) + 1, len(near)):
        spread(k)
    for i in range(count_of + LAG):
        if i < count_of:
            s2_start(i)
        if i + AHEAD < count_of:
            local_sum(i + AHEAD)
            s1_start(i + AHEAD)
        if i == LAG:
            spread(len(near))
        if 0 <= i - LAG < count_of:
            s3_start(i - LAG)
    for done, copies in ((foot_v, 3), (morph_ref, 4)):
        pltpu.make_async_copy(done, done, side_sem.at[copies]).wait()
    for q in range(chunks):
        finish(q)

    update(0)
    for it in range(1, ITERS):
        steps()
        acc[...] = jnp.zeros_like(acc)

        def again(i, carry):
            deblend(i * (group * LANES), False)
            return carry

        lax.fori_loop(0, block // (group * LANES), again, 0)
        update(it)
    for c in range(bands):
        out = spectra[0, c]
        for k in range(1, slots):
            out = jnp.where(lane == k, spectra[k, c], out)
        spec_out[c] = out[0:owned, :slots]

    gone = sums.at[:, pl.ds(1, ne - 1)]
    pltpu.make_async_copy(gone, gone, send_sem.at[3]).wait()


def hand_over(coadd_in, spec_in, morph_in, coadd_out, spec_out, morph_out, sems):
    owned, _, pix_part = morph_out.shape
    _, held, block = morph_in.shape
    for row in range(held):
        pltpu.make_async_copy(
            morph_in.at[:, row, :],
            morph_out.at[row % owned, :, pl.ds(row // owned * block, block)], sems.at[2]).start()
    others = [pltpu.make_async_copy(coadd_in, coadd_out, sems.at[0]),
              pltpu.make_async_copy(spec_in, spec_out, sems.at[1])]
    for copy in others:
        copy.start()
    pltpu.make_async_copy(morph_in, morph_in, sems.at[2]).wait()
    for copy in others:
        copy.wait()


def fused(ne, nb, visit_flux, visit_precision, visit_live, footprint, source_count, spectra_init,
          morphology_init):
    visits, every_blend, bands, block = visit_flux.shape
    owned, slots, pix_part = morphology_init.shape
    width = ne * LANES
    chunks = block // width
    per_dest = pix_part // block
    held = per_dest * owned
    count_of = len(cut(chunks, bands))
    loads = count_of // chunks + chunks - 1
    slot_count = plan()[1]
    f32 = jnp.float32
    vmem, hbm = (pl.BlockSpec(memory_space=s) for s in (pltpu.VMEM, pl.ANY))
    dma = pltpu.SemaphoreType.DMA
    parts = pl.pallas_call(
        functools.partial(coadd_kernel, ne=ne, nb=nb),
        out_shape=(
            pltpu.VMEM((bands, owned, pix_part), f32),
            pltpu.VMEM((bands, owned, slots), f32),
            pltpu.VMEM((slots, held, block), f32),
        ),
        in_specs=[hbm] * 7,
        out_specs=(vmem, vmem, vmem),
        scratch_shapes=[
            pltpu.VMEM((2, chunks, visits, bands, every_blend, width), visit_flux.dtype),
            pltpu.VMEM(visit_live.shape, jnp.int32),
            pltpu.VMEM((slots, held, block), jnp.int32),
            pltpu.SMEM(source_count.shape, jnp.int32),
            pltpu.VMEM((bands, owned, slots), f32),
            pltpu.VMEM((bands, held, block), f32),
            pltpu.VMEM((bands, held, block), f32),
            pltpu.VMEM((chunks, slot_count, bands, held, LANES), f32),
            pltpu.VMEM((chunks, slot_count, bands, held, LANES), f32),
            pltpu.VMEM((chunks, slot_count, bands, held, LANES), f32),
            pltpu.VMEM((chunks, per_dest, slot_count, bands, owned, LANES), f32),
            pltpu.VMEM((chunks, per_dest, 2 * ne, bands, owned, LANES), f32),
            pltpu.VMEM((slots, bands, held, LANES), f32),
            pltpu.VMEM((slots, held, LANES), f32),
            pltpu.VMEM((slots, bands + 1, held, LANES), f32),
            pltpu.VMEM((ITERS, ne, held, LANES), f32),
            dma((loads,)),
            dma((5,)),
            pltpu.SemaphoreType.REGULAR((len(bits(ne)) + len(bits(nb)) - 1,)),
            dma((4,)),
            dma((count_of,)),
            dma((count_of,)),
            dma((chunks,)),
            dma((ITERS,)),
        ],
        compiler_params=pltpu.CompilerParams(
            collective_id=0, has_side_effects=True, vmem_limit_bytes=58 * 2**20
        ),
    )(visit_flux.transpose(0, 2, 1, 3), visit_precision.transpose(0, 2, 1, 3), visit_live,
      footprint, source_count, spectra_init.transpose(2, 0, 1), morphology_init)
    coadd, spectra, morphology = pl.pallas_call(
        hand_over,
        out_shape=(
            jax.ShapeDtypeStruct((bands, owned, pix_part), f32),
            jax.ShapeDtypeStruct((bands, owned, slots), f32),
            jax.ShapeDtypeStruct((owned, slots, pix_part), f32),
        ),
        in_specs=[vmem] * 3,
        out_specs=(hbm,) * 3,
        scratch_shapes=[dma((3,))],
        compiler_params=pltpu.CompilerParams(vmem_limit_bytes=8 * 2**20),
    )(*parts)
    return coadd.transpose(1, 0, 2), spectra.transpose(1, 2, 0), morphology


def on_device(
    visit_flux, visit_precision, visit_live, footprint, source_count, spectra_init, morphology_init
):
    weights = visit_precision.astype(jnp.float32) * visit_live.astype(jnp.float32)[:, :, None, None]
    numerator = jnp.sum(weights * visit_flux.astype(jnp.float32), axis=0)
    weight_sum = jnp.sum(weights, axis=0)
    pix_part = morphology_init.shape[2]
    owned = morphology_init.shape[0]
    numerator, weight_sum = (
        lax.psum_scatter(numerator, "epoch", scatter_dimension=2, tiled=True),
        lax.psum_scatter(weight_sum, "epoch", scatter_dimension=2, tiled=True),
    )
    every_blend, band_count, piece = numerator.shape
    numerator = numerator.reshape(every_blend, band_count, 1, piece)
    weight_sum = weight_sum.reshape(every_blend, band_count, 1, piece)
    numerator, weight_sum = (
        lax.all_to_all(numerator, "blend", split_axis=0, concat_axis=2, tiled=True),
        lax.all_to_all(weight_sum, "blend", split_axis=0, concat_axis=2, tiled=True),
    )
    blocks = numerator.shape[2]
    numerator = numerator.reshape(owned, band_count, blocks, 1, piece)
    weight_sum = weight_sum.reshape(owned, band_count, blocks, 1, piece)
    numerator, weight_sum = (
        lax.all_to_all(numerator, "epoch", split_axis=2, concat_axis=3, tiled=True),
        lax.all_to_all(weight_sum, "epoch", split_axis=2, concat_axis=3, tiled=True),
    )
    numerator = numerator.reshape(owned, band_count, pix_part)
    weight_sum = weight_sum.reshape(owned, band_count, pix_part)
    coadd_flux = numerator / (1.0 + weight_sum)
    coverage = weight_sum / (1.0 + weight_sum)
    slots = footprint.shape[1]
    source_live = (jnp.arange(slots, dtype=jnp.int32)[None, :] < source_count[:, None]).astype(
        jnp.float32
    )
    footprint_mask = footprint.astype(jnp.float32) * source_live[:, :, None]
    live_count = source_count.astype(jnp.float32)
    morphology = morphology_init * footprint_mask
    spectra = spectra_init
    highest = lax.Precision.HIGHEST
    for iteration in range(ITERS):
        blend_model = jnp.einsum("bkc,bkp->bcp", spectra, morphology, precision=highest)
        residual = coverage * (coadd_flux - blend_model)
        morph_grad = jnp.einsum("bkc,bcp->bkp", spectra, residual, precision=highest)
        morph_step = 1.0 / (1.0 + live_count[:, None] * jnp.sum(spectra * spectra, axis=2))
        morphology = (
            jnp.maximum(0.0, morphology + morph_grad * morph_step[:, :, None]) * footprint_mask
        )
        blend_model = jnp.einsum("bkc,bkp->bcp", spectra, morphology, precision=highest)
        residual = coverage * (coadd_flux - blend_model)
        spectra_grad = jnp.einsum("bkp,bcp->bkc", morphology, residual, precision=highest)
        morph_norm = jnp.sum(morphology * morphology, axis=2)
        spectra_grad, morph_norm = lax.psum((spectra_grad, morph_norm), "epoch")
        spectra = jnp.maximum(
            0.0, spectra + spectra_grad / (1.0 + live_count[:, None] * morph_norm)[:, :, None]
        )
    return (coadd_flux, spectra, morphology)


def solution(mesh):
    ne, nb = mesh.shape["epoch"], mesh.shape["blend"]

    def step(visit_flux, visit_precision, visit_live, footprint, source_count, spectra_init,
             morphology_init):
        block, bands = visit_flux.shape[3], visit_flux.shape[2]
        owned, pix_part = morphology_init.shape[0], morphology_init.shape[2]
        fits = (
            block % (ne * LANES) == 0
            and pix_part % block == 0
            and factors(ne) == (2, 2)
            and nb == 2 * ne
            and pix_part == 2 * block
            and visit_flux.shape[1] == owned * nb
            and AHEAD <= block // (ne * LANES) * bands
            and morphology_init.shape[1] * (bands + 1) <= LANES
        )
        run = functools.partial(fused, ne, nb) if fits else on_device
        return run(visit_flux, visit_precision, visit_live, footprint, source_count, spectra_init,
                   morphology_init)

    in_specs = (
        P("epoch", None, None, "blend"),
        P("epoch", None, None, "blend"),
        P("epoch", None),
        P("blend", None, "epoch"),
        P("blend"),
        P("blend", None, None),
        P("blend", None, "epoch"),
    )
    out_specs = (P("blend", None, "epoch"), P("blend", None, None), P("blend", None, "epoch"))
    return jax.shard_map(
        step, mesh=mesh, in_specs=in_specs, out_specs=out_specs, check_vma=False
    )
```
